32 devices in a mesh: group: 8 (over z, x), tensor: 4 (over y, core).
Axes of the slice: x: 2, y: 2, z: 4, core: 2. Of those that a mesh axis runs over, the one named last changes fastest.
Arguments:
- queries: bfloat16 [64, 64, 5120], P('group', None, 'tensor'), may hold values from -15 to 15
- prefix_keys: bfloat16 [16, 1024, 1024], P('group', None, 'tensor'), may hold values from -200 to 200
- prefix_values: bfloat16 [16, 1024, 1024], P('group', None, 'tensor'), may hold values from -6 to 6
- slot_of_prompt: int32 [16], replicated, may hold values from 0 to 15, as said below
- prompt_of: int32 [64], P('group'), may hold values from 0 to 15, as said below
- lengths: int32 [64], P('group'), may hold values from 1 to 64
Outputs:
- attended: bfloat16 [64, 64, 5120], P('group', 'tensor')
The draws below stay inside these ranges and needn't reach their ends.
Inputs may be any that keep to these rules, and one draw needn't show every extreme that they name: A permutation: prompt p's keys and values lie in row slot_of_prompt[p] of the prefix arrays, and that row belongs to group index slot_of_prompt[p] // 2. `prompt_of`: of the 8 completions on one group index, at most 2 have prompts cached on any one group index, and on every group index some group index caches the prompts of exactly 2 of them.
All inputs are finite; a program needn't handle non-finite values.
Results may differ from the reference program's by a relative error of at most 0.012.
Values may be sent and summed in bfloat16 or wider, within the bound.
A program may use at most 128 MiB of HBM per device.

```python
import math
import jax
import jax.numpy as jnp
from jax import lax

D = 5120
HEADS = 40
KV_HEADS = 8
HEAD = 128
PREFIX = 1024
COMP = 64
CAPC = 2
PPG = 2
CPD = 8
COMPLETIONS = 64
PROMPTS = 16


def routing_tables(key):
    base = jax.random.fold_in(key, 4217)
    first_key, second_key = jax.random.split(base, 2)
    slot_of_prompt = jax.random.permutation(first_key, PROMPTS).astype(jnp.int32)
    prompt_at = jnp.argsort(slot_of_prompt, stable=True).astype(jnp.int32)
    blocks = COMPLETIONS // CPD
    block_keys = jax.random.split(second_key, blocks)

    def one_block(block_key):
        key_spare, key_order, key_offset, key_local = jax.random.split(block_key, 4)
        spare = CAPC + jax.random.permutation(key_spare, blocks * CAPC - CAPC)
        chosen = jnp.concatenate([jnp.arange(CAPC), spare[:CPD - CAPC]])
        chosen = jax.random.permutation(key_order, chosen)
        offset = jax.random.randint(key_offset, (), 0, blocks)
        owner_group = (chosen // CAPC + offset) % blocks
        local_rows = jax.random.randint(key_local, (CPD,), 0, PPG)
        return owner_group * PPG + local_rows
    cache_slots = jax.vmap(one_block)(block_keys).reshape(COMPLETIONS)
    prompt_of = prompt_at[cache_slots].astype(jnp.int32)
    return (slot_of_prompt, prompt_of)


def draw_slot_of_prompt(key, part):
    return routing_tables(key)[0]


def draw_prompt_of(key, part):
    return routing_tables(key)[1]


def draw_prefix_keys(key, part):
    base = jax.random.fold_in(key, 913)
    key_base = jax.random.fold_in(base, 0)
    entries = jax.random.normal(key_base, (PROMPTS, PREFIX, KV_HEADS, HEAD), jnp.float32)
    entries = jnp.clip(entries, -200.0, 200.0)
    return entries.reshape(PROMPTS, PREFIX, KV_HEADS * HEAD).astype(jnp.bfloat16)


def place_ends(array, stream_key, smallest, largest):
    dims = array.shape
    spot = [jax.random.randint(jax.random.fold_in(stream_key, axis), (), 0, dims[axis]) for axis in range(len(dims))]
    array = array.at[tuple(spot)].set(smallest)
    longest = dims.index(max(dims))
    spot[longest] = (spot[longest] + 1) % dims[longest]
    return array.at[tuple(spot)].set(largest)


def shard_levels(stream_key, shape, cuts, smallest, largest):
    level = 1.0
    for position, blocks in cuts:
        draws = jax.random.uniform(jax.random.fold_in(jax.random.fold_in(stream_key, 6), position), (blocks,), jnp.float32, smallest / len(cuts), largest / len(cuts))
        level = level * jnp.repeat(jnp.exp(draws), shape[position] // blocks).reshape((-1,) + (1,) * (len(shape) - 1 - position))
    return level


def bell_draw(rng, shape, deviation, limit, pieces=(), kind=jnp.bfloat16):
    values = deviation * jax.random.normal(rng, shape, jnp.float32)
    if pieces:
        values = values * shard_levels(rng, shape, pieces, -0.22, 0.18)
    return jnp.clip(values, -limit, limit).astype(kind)


def setup_inputs(seed: int = 0) -> dict:
    key_list = jax.random.split(jax.random.key(seed), 7)
    queries = bell_draw(key_list[0], (COMPLETIONS, COMP, D), 2.5, 15.0, ((0, 8), (2, 4)))
    prefix_keys = draw_prefix_keys(jax.random.fold_in(key_list[6], 71), 0)
    prefix_values = bell_draw(key_list[2], (PROMPTS, PREFIX, KV_HEADS * HEAD), 1.0, 6.0, ((0, 8), (2, 4)))
    slot_of_prompt = draw_slot_of_prompt(jax.random.fold_in(key_list[6], 71), 0)
    prompt_of = draw_prompt_of(jax.random.fold_in(key_list[6], 71), 0)
    lengths = place_ends(jax.random.randint(key_list[5], (COMPLETIONS,), 1, COMP + 1), jax.random.fold_in(key_list[5], 1), 1, COMP).astype(jnp.int32)
    return dict(queries=queries, prefix_keys=prefix_keys, prefix_values=prefix_values, slot_of_prompt=slot_of_prompt, prompt_of=prompt_of, lengths=lengths)


rotary_base = 1000000.0

def rotary(head_rows, positions):
    half_dim = head_rows.shape[-1] // 2
    frequencies = rotary_base ** (-(jnp.arange(half_dim, dtype=jnp.float32) * 2.0 / head_rows.shape[-1]))
    angles = positions[:, None] * frequencies[None, :]
    cos_table = jnp.cos(angles)[:, None, :]
    sin_table = jnp.sin(angles)[:, None, :]
    first_half = head_rows[..., :half_dim]
    second_half = head_rows[..., half_dim:]
    return jnp.concatenate([first_half * cos_table - second_half * sin_table, second_half * cos_table + first_half * sin_table], axis=-1)

def reference(queries, prefix_keys, prefix_values, slot_of_prompt, prompt_of, lengths):
    positions = (PREFIX + jnp.arange(COMP)).astype(jnp.float32)
    cache_rows = slot_of_prompt[prompt_of].astype(jnp.int32)
    per_kv = HEADS // KV_HEADS
    scaling = 1.0 / math.sqrt(HEAD)
    highest = lax.Precision.HIGHEST

    def single(inputs):
        query_rows, cache_row, length = inputs
        roped = rotary(query_rows.astype(jnp.float32).reshape(COMP, HEADS, HEAD), positions).astype(jnp.bfloat16)
        grouped = roped.astype(jnp.float32).reshape(COMP, KV_HEADS, per_kv, HEAD)
        cached_keys = lax.dynamic_index_in_dim(prefix_keys, cache_row, 0, keepdims=False).astype(jnp.float32).reshape(PREFIX, KV_HEADS, HEAD)
        cached_values = lax.dynamic_index_in_dim(prefix_values, cache_row, 0, keepdims=False).astype(jnp.float32).reshape(PREFIX, KV_HEADS, HEAD)
        scores = jnp.einsum('rkgd,pkd->kgrp', grouped, cached_keys, precision=highest) * scaling
        peak = lax.optimization_barrier(jnp.max(scores, axis=-1, keepdims=True))
        weights = jnp.exp(scores - peak)
        denominator = lax.optimization_barrier(jnp.sum(weights, axis=-1))
        probabilities = weights.astype(jnp.bfloat16).astype(jnp.float32)
        weighted = jnp.einsum('kgrp,pkd->rkgd', probabilities, cached_values, precision=highest)
        attended = (weighted / jnp.transpose(denominator, (2, 0, 1))[..., None]).astype(jnp.bfloat16).reshape(COMP, D)
        live_rows = jnp.arange(COMP) < length
        return jnp.where(live_rows[:, None], attended, jnp.zeros_like(attended))
    return lax.map(single, (queries, cache_rows, lengths))
```

```python
import functools
import math

import numpy as np

import jax
import jax.numpy as jnp
from jax import lax
from jax.experimental import pallas as pl
from jax.experimental.pallas import tpu as pltpu
from jax.sharding import PartitionSpec as P

HEAD = 128
CAPC = 2
ROTARY_BASE = 1000000.0
TILE = 16
UNIT = 8
BATCH = 4
LANES = 128
MESH = pl.DeviceIdType.MESH
LEVELS = ((0.625, 0.47), (0.6875, 0.532), (0.75, 0.594), (0.875, 0.6875), (1.0, 1.0))


def rotary_tables(first_position, rows):
    half = HEAD // 2
    frequencies = np.float32(ROTARY_BASE) ** (
        -(np.arange(half, dtype=np.float32) * np.float32(2.0) / np.float32(HEAD))
    )
    positions = (first_position + np.arange(rows)).astype(np.float32)
    angles = (positions[:, None] * frequencies.astype(np.float32)[None, :]).astype(np.float64)
    cos, sin = np.cos(angles), np.sin(angles)
    return (
        np.concatenate([cos, cos], axis=1).astype(np.float32),
        np.concatenate([-sin, sin], axis=1).astype(np.float32),
    )


def padded_kernel(
    groups, lanes, moved,
    source_ref, tag_ref, dest_ref, length_ref,
    q_ref, k_ref, v_ref, cos_ref, sin_ref,
    out_ref,
    q_out, q_in, sel_out, sel_in, res, stage,
    q_send, q_recv, s_send, s_recv, r_send, r_recv,
    *near,
):
    me, lane = lax.axis_index("group"), lax.axis_index("tensor")
    held, rows, width = q_ref.shape
    cached, prefix, kv_width = k_ref.shape
    share = rows // lanes
    kv_local = kv_width // HEAD
    per_kv = width // HEAD // kv_local
    half = groups // 2
    factor = math.log2(math.e) / math.sqrt(HEAD)
    wide_near = moved * per_kv * HEAD
    if moved:
        (n_out, n_in, ns_out, ns_in, n_res, k_far, v_far,
         n_send, n_recv, ns_send, ns_recv, nr_send, nr_recv, kv_send, kv_recv) = near
    spot = lax.rem(me, half)
    base = me - spot
    mirror = lax.rem(me + half, groups)

    barrier = pltpu.get_barrier_semaphore()

    def greet(step, carry):
        for turn in range(lanes):
            def send():
                pl.semaphore_signal(
                    barrier, inc=1,
                    device_id=(lax.rem(me + step, groups), lax.rem(lane + turn, lanes)),
                    device_id_type=MESH,
                )
            if turn:
                send()
            else:
                pl.when(step > 0)(send)
        return carry

    lax.fori_loop(0, groups, greet, 0)

    def offset_of(step):
        swing = (step + 1) // 2
        return lax.rem(half + (1 - 2 * lax.rem(step, 2)) * swing + groups, groups)

    def route(owner):
        places = [owner * CAPC + slot for slot in range(CAPC)]
        return [(source_ref[place], tag_ref[place]) for place in places]

    def fill(items, q_to, sel_to, block, first, last):
        for slot, (item, tag) in enumerate(items):
            for j in range(cached):
                weight = jnp.where(tag == j, 1.0, 0.0)
                sel_to[block, slot * cached + j] = jnp.full(
                    (TILE, HEAD), weight, jnp.float32
                ).astype(jnp.bfloat16)
            for head in range(first, last):
                x = q_ref[item, :, head * HEAD:(head + 1) * HEAD].astype(jnp.float32)
                turned = x * cos_ref[...] + pltpu.roll(x, HEAD // 2, 1) * sin_ref[...]
                span = slice((head - first) * HEAD, (head - first + 1) * HEAD)
                q_to[block, slot, :, span] = turned.astype(jnp.bfloat16)

    near_heads, all_heads = moved * per_kv, width // HEAD

    def pair(src, dst, send_sem, recv_sem, device):
        return pltpu.make_async_remote_copy(
            src_ref=src, dst_ref=dst, send_sem=send_sem, recv_sem=recv_sem,
            device_id=device, device_id_type=MESH,
        )

    def q_copies(here, there, device):
        return (
            pair(sel_out.at[here], sel_in.at[there], s_send.at[here], s_recv.at[there],
                 (device, lane)),
            pair(q_out.at[here], q_in.at[there], q_send.at[here], q_recv.at[there],
                 (device, lane)),
        )

    def n_copies(here, there, device):
        return (
            pair(ns_out.at[here], ns_in.at[there], ns_send.at[here], ns_recv.at[there],
                 (device, lane)),
            pair(n_out.at[here], n_in.at[there], n_send.at[here], n_recv.at[there],
                 (device, lane)),
        )

    def place(owner, from_lane, skip, wide):
        start = pl.multiple_of(from_lane * width + skip, HEAD)
        return stage.at[pl.ds(owner * CAPC, CAPC), :, pl.ds(start, wide)]

    def r_copy(block, piece, owner, from_lane, device):
        return pair(
            res.at[block, :, piece], place(owner, from_lane, wide_near, width - wide_near),
            r_send.at[block, piece], r_recv.at[owner, from_lane], (device, piece),
        )

    def nr_copy(block, piece, owner, from_lane, device):
        return pair(
            n_res.at[block, :, piece], place(owner, from_lane, 0, wide_near),
            nr_send.at[block, piece], nr_recv.at[owner, from_lane], (device, piece),
        )

    def kv_copies():
        span = pl.ds(0, moved * HEAD)
        return (
            pair(k_ref.at[:, :, span], k_far, kv_send.at[0], kv_recv.at[0], (mirror, lane)),
            pair(v_ref.at[:, :, span], v_far, kv_send.at[1], kv_recv.at[1], (mirror, lane)),
        )

    items = route(mirror)
    fill(items, q_out, sel_out, mirror, near_heads, all_heads)
    pl.semaphore_wait(barrier, groups * lanes - 1)
    for copy in q_copies(mirror, me, mirror):
        copy.start()
    if moved:
        fill(items, n_in, ns_in, spot + half, 0, near_heads)

    def dispatch(step, carry):
        owner = lax.rem(me + offset_of(step), groups)
        items = route(owner)
        fill(items, q_out, sel_out, owner, near_heads, all_heads)
        for copy in q_copies(owner, me, owner):
            copy.start()
        if moved:
            fill(items, n_out, ns_out, owner, 0, near_heads)
            seat = lax.rem(owner, half)
            kind = lax.rem(lax.div(owner, half) + lax.div(me, half), 2)
            for copy in n_copies(owner, spot + half * kind, base + seat):
                copy.start()
        return carry

    lax.fori_loop(1, groups - 1, dispatch, 0)
    if moved:
        for copy in kv_copies():
            copy.start()
    items = route(me)
    fill(items, q_in, sel_in, me, near_heads, all_heads)
    if moved:
        fill(items, n_in, ns_in, spot, 0, near_heads)

    def attend(q_from, sel_from, to, block, keys, values, first, count):
        for slot in range(CAPC):
            weights = [sel_from[block, slot * cached + j][None] for j in range(cached)]

            def chosen(ref, span):
                total = None
                for j in range(cached):
                    part = ref[j, :, span].reshape(prefix // TILE, TILE, HEAD) * weights[j]
                    total = part if total is None else total + part
                return total.reshape(prefix, HEAD)

            for kv in range(count):
                span = slice((first + kv) * HEAD, (first + kv + 1) * HEAD)
                spans = [
                    slice((kv * per_kv + g) * HEAD, (kv * per_kv + g + 1) * HEAD)
                    for g in range(per_kv)
                ]
                query = jnp.concatenate([q_from[block, slot, :, s] for s in spans], axis=0)
                scores = lax.dot_general(
                    query, chosen(keys, span), (((1,), (1,)), ((), ())),
                    preferred_element_type=jnp.float32,
                )
                peak = jnp.max(scores, axis=-1, keepdims=True)
                weight = jnp.exp2((scores - peak) * factor)
                total = jnp.sum(weight, axis=-1, keepdims=True)
                mixed = jnp.dot(
                    weight.astype(jnp.bfloat16), chosen(values, span),
                    preferred_element_type=jnp.float32,
                )
                mixed = (mixed / total).astype(jnp.bfloat16)
                for g in range(per_kv):
                    to[block, slot, :, :, spans[g]] = mixed[g * rows:(g + 1) * rows].reshape(
                        lanes, share, HEAD
                    )

    def give_back(step, copy, source, block, owner, done, skip, wide):
        for turn in range(1, lanes):
            copy(block, lax.rem(lane + turn, lanes), owner, lane, source).start()

        @pl.when(step > 0)
        def _():
            copy(block, lane, owner, lane, source).start()

        @pl.when(step == 0)
        def _():
            start = pl.multiple_of(lane * width + skip, HEAD)
            stage[pl.ds(owner * CAPC, CAPC), :, pl.ds(start, wide)] = done[block, :, lane]

    def far_work(step, carry):
        source = lax.rem(me + groups - offset_of(lax.rem(step + groups - 1, groups)), groups)

        @pl.when(step > 0)
        def _():
            for copy in q_copies(source, source, source):
                copy.wait_recv()

        attend(q_in, sel_in, res, source, k_ref, v_ref, moved, kv_local - moved)
        give_back(step, r_copy, source, source, me, res, wide_near, width - wide_near)
        return carry

    def near_work(kind, keys, values, owner):
        def body(step, carry):
            seat = lax.rem(spot + step, half)
            block = seat + half * kind

            @pl.when(step > 0)
            def _():
                for copy in n_copies(block, block, base + seat):
                    copy.wait_recv()

            attend(n_in, ns_in, n_res, block, keys, values, 0, moved)
            give_back(step, nr_copy, base + seat, block, owner, n_res, 0, wide_near)
            return carry

        lax.fori_loop(0, half, body, 0)

    if moved:
        near_work(0, k_ref, v_ref, me)
    lax.fori_loop(0, groups, far_work, 0)
    if moved:
        for copy in kv_copies():
            copy.wait_recv()
        near_work(1, k_far, v_far, mirror)

    def returned(step, copy, block, owner, device):
        @pl.when(step > 0)
        def _():
            copy(block, lane, owner, lane, device).wait_send()
            copy(block, lane, owner, lane, device).wait_recv()

        for turn in range(1, lanes):
            piece = lax.rem(lane + turn, lanes)
            copy(block, piece, owner, piece, device).wait_send()
            copy(block, piece, owner, piece, device).wait_recv()

    def far_settle(step, carry):
        other = lax.rem(me + step, groups)

        @pl.when(step > 0)
        def _():
            for copy in q_copies(other, me, other):
                copy.wait_send()

        returned(step, r_copy, other, other, other)
        return carry

    lax.fori_loop(0, groups, far_settle, 0)
    if moved:
        for copy in kv_copies():
            copy.wait_send()

        def near_settle(step, carry):
            seat = lax.rem(spot + step, half)
            for kind in range(2):
                owner = lax.rem(base + half * kind, groups) + seat

                @pl.when(step > 0)
                def _():
                    for copy in n_copies(owner, owner, base + seat):
                        copy.wait_send()

                returned(step, nr_copy, seat + half * kind, owner, base + seat)
            return carry

        lax.fori_loop(0, half, near_settle, 0)

    def deliver(item, carry):
        found = stage[dest_ref[item]].astype(jnp.float32)
        position = lane * share + lax.broadcasted_iota(jnp.int32, found.shape, 0)
        out_ref[item] = jnp.where(position < length_ref[item], found, 0.0).astype(jnp.bfloat16)
        return carry

    lax.fori_loop(0, held, deliver, 0)


def padded(groups, lanes, queries, prefix_keys, prefix_values, slot_of_prompt, prompt_of, lengths):
    held, rows, width = queries.shape
    cached, prefix, kv_width = prefix_keys.shape
    share = rows // lanes
    kv_local = kv_width // HEAD
    moved = kv_local // 2 if groups % 2 == 0 and groups >= 4 else 0
    wide_near = moved * (width // kv_local)
    wide = width - wide_near
    cos, sin = rotary_tables(prefix, rows)
    cache_rows = slot_of_prompt[prompt_of]
    owner = cache_rows // cached
    serial = jnp.arange(held)
    earlier = (owner[None, :] == owner[:, None]) & (serial[None, :] < serial[:, None])
    destination = owner * CAPC + jnp.sum(earlier.astype(jnp.int32), axis=1)
    matches = destination[None, :] == jnp.arange(groups * CAPC)[:, None]
    source = jnp.sum(jnp.where(matches, serial[None, :], 0), axis=1)
    tags = jnp.sum(jnp.where(matches, (cache_rows % cached)[None, :], 0), axis=1)
    smem = pl.BlockSpec(memory_space=pltpu.SMEM)
    vmem = pl.BlockSpec(memory_space=pltpu.VMEM)
    dma = pltpu.SemaphoreType.DMA
    bf16 = jnp.bfloat16

    def exchange(features):
        return [
            pltpu.VMEM((groups, CAPC, rows, features), bf16),
            pltpu.VMEM((groups, CAPC, rows, features), bf16),
            pltpu.VMEM((groups, CAPC * cached, TILE, HEAD), bf16),
            pltpu.VMEM((groups, CAPC * cached, TILE, HEAD), bf16),
            pltpu.VMEM((groups, CAPC, lanes, share, features), bf16),
        ]

    semaphores = [
        dma((groups,)), dma((groups,)),
        dma((groups,)), dma((groups,)),
        dma((groups, lanes)), dma((groups, lanes)),
    ]
    scratch = [
        *exchange(wide),
        pltpu.VMEM((groups * CAPC, share, width * lanes), bf16),
        *semaphores,
    ]
    if moved:
        scratch += [
            *exchange(wide_near),
            pltpu.VMEM((cached, prefix, moved * HEAD), bf16),
            pltpu.VMEM((cached, prefix, moved * HEAD), bf16),
            *semaphores,
            dma((2,)), dma((2,)),
        ]
    return pl.pallas_call(
        functools.partial(padded_kernel, groups, lanes, moved),
        out_shape=jax.ShapeDtypeStruct((held, share, width * lanes), bf16),
        in_specs=[smem] * 4 + [vmem] * 5,
        out_specs=vmem,
        scratch_shapes=scratch,
        compiler_params=pltpu.CompilerParams(collective_id=0, has_side_effects=True),
        name="routed_prefix_attention",
    )(
        source.astype(jnp.int32), tags.astype(jnp.int32), destination.astype(jnp.int32), lengths,
        queries, prefix_keys, prefix_values, jnp.asarray(cos), jnp.asarray(sin),
    )


def xor_order(step, plane, planes):
    half = planes // 2
    near = lax.div(step, half)
    side = lax.rem(lax.div(plane, half) + 1 - near, 2)
    return side * half + lax.rem(lax.rem(plane, half) + step + near, half)


def plan_kernel(
    groups, pair, levels, full, batches,
    slot_ref, prompt_ref, length_ref,
    tables_ref,
    mine, gathered, send, recv,
):
    me, lane = lax.axis_index("group"), lax.axis_index("tensor")
    held = prompt_ref.shape[0]
    slots = slot_ref.shape[0]
    planes = groups // pair
    per_plane = slots // planes
    total = groups * held
    full_pair, full_plane = full
    barrier = pltpu.get_barrier_semaphore()

    def greet(step, carry):
        pl.semaphore_signal(
            barrier, inc=1, device_id=(lax.rem(me + step, groups), lane), device_id_type=MESH
        )
        return carry

    lax.fori_loop(1, groups, greet, 0)
    lanes1 = lax.broadcasted_iota(jnp.int32, (1, LANES), 1)
    row = jnp.zeros((1, LANES), jnp.int32)
    for i in range(held):
        value = slot_ref[prompt_ref[i]] * LANES + length_ref[i]
        row = jnp.where(lanes1 == me * held + i, value, row)
    mine[...] = row
    gathered[me] = row
    pl.semaphore_wait(barrier, groups - 1)

    def copy(there, device):
        return pltpu.make_async_remote_copy(
            src_ref=mine, dst_ref=gathered.at[there], send_sem=send.at[device],
            recv_sem=recv.at[there], device_id=(device, lane), device_id_type=MESH,
        )

    def push(step, carry):
        copy(me, lax.rem(me + step, groups)).start()
        return carry

    lax.fori_loop(1, groups, push, 0)

    def settle(step, carry):
        other = lax.rem(me + step, groups)
        copy(other, other).wait_recv()
        copy(me, other).wait_send()
        return carry

    lax.fori_loop(1, groups, settle, 0)
    code = gathered[0]
    for g in range(1, groups):
        code = code + gathered[g]

    square = (LANES, LANES)
    down = lax.broadcasted_iota(jnp.int32, square, 0)
    across = lax.broadcasted_iota(jnp.int32, square, 1)
    eye = down == across

    def to_column(values):
        return jnp.sum(jnp.where(eye, jnp.broadcast_to(values, square), 0), axis=1, keepdims=True)

    def to_row(values):
        return jnp.sum(jnp.where(eye, jnp.broadcast_to(values, square), 0), axis=0, keepdims=True)

    def facts(values, index):
        live = index < total
        length = values % LANES
        slot = values // LANES
        count = jnp.where(live, (length + UNIT - 1) // UNIT, 0)
        return count, slot, slot // per_plane, index // held, index // (held * pair)

    col = to_column(code)
    down1 = lax.broadcasted_iota(jnp.int32, (LANES, 1), 0)
    count_r, slot_r, to_r, from_r, plane_r = facts(code, lanes1)
    count_c, slot_c, to_c, from_c, plane_c = facts(col, down1)
    weight = jnp.broadcast_to(count_c, square)
    earlier = (down < across) & (to_c == to_r)

    def rank(mask):
        return jnp.sum(jnp.where(mask, weight, 0), axis=0, keepdims=True)

    base1 = rank(earlier & (from_c == from_r))
    base2 = rank(earlier & (plane_c == plane_r))
    within = rank(earlier & (plane_c == plane_r) & (slot_c == slot_r))
    key_r = plane_r * slots + slot_r
    number = jnp.sum(
        jnp.where(down1 == key_r, jnp.broadcast_to(count_r, square), 0), axis=1, keepdims=True
    )
    need = (number + BATCH - 1) // BATCH
    need_r = to_row(need)
    first = jnp.sum(
        jnp.where(
            (down // per_plane == across // per_plane) & (across < down),
            jnp.broadcast_to(need_r, square), 0,
        ),
        axis=1, keepdims=True,
    )
    first_of = jnp.sum(
        jnp.where(down1 == key_r, jnp.broadcast_to(first, square), 0), axis=0, keepdims=True
    )
    place = first_of * BATCH + within
    base1_c, base2_c, place_c = to_column(base1), to_column(base2), to_column(place)

    z = me // pair
    wide1 = jnp.max(jnp.where(lanes1 < total, base1 + count_r, 0), keepdims=True)
    wide2 = jnp.max(jnp.where(lanes1 < total, base2 + count_r, 0), keepdims=True)
    level = jnp.zeros((1, 1), jnp.int32)
    for cap1, cap2 in levels[:-1]:
        level = level + jnp.where((wide1 > cap1) | (wide2 > cap2), 1, 0)
    tables_ref[pl.ds(0, 1), :] = jnp.broadcast_to(level, (1, LANES))
    tables_ref[pl.ds(1, 1), :] = code
    tables_ref[pl.ds(2, 1), :] = to_r * full_plane + base2

    def pick(mask, start_c, value_c, index):
        hit = mask & (index >= start_c) & (index < start_c + count_c)
        return jnp.sum(jnp.where(hit, value_c + index, 0), axis=0, keepdims=True)

    for plane in range(planes):
        tables_ref[pl.ds(3 + plane, 1), :] = pick(
            (from_c == me) & (to_c == plane), base1_c,
            lax.rem(down1, held) * (full_pair // (CAPC * pair)) - base1_c, lanes1,
        )
        here = (plane_c == plane) & (to_c == z)
        tables_ref[pl.ds(3 + planes + plane, 1), :] = pick(
            here, place_c, lax.rem(from_c, pair) * full_pair + base1_c - place_c, lanes1
        )
        tables_ref[pl.ds(3 + 2 * planes + plane, 1), :] = pick(
            here, base2_c, place_c - base2_c, lanes1
        )
        starts = (
            (down1 // slots == plane) & (lax.rem(down1, slots) // per_plane == z)
            & (lanes1 >= first) & (lanes1 < first + need)
        )
        tables_ref[pl.ds(3 + 3 * planes + plane, 1), :] = jnp.sum(
            jnp.where(starts, lax.rem(down1, per_plane), 0), axis=0, keepdims=True
        )


def packed_kernel(
    groups, lanes, pair, full, cap1, cap2, batches,
    tables,
    q_ref, k_ref, v_ref, cos_ref, sin_ref,
    out_ref,
    q_out, q_in, k_all, v_all, results, r_out_a, r_out_b, r_in_a, r_in_b, stage_a, stage_b,
    q_send, q_recv, kv_send, kv_recv, kv_here,
    ra_send, ra_recv, rb_send, rb_recv, fa_send, fa_recv, fb_send, fb_recv,
):
    me, lane = lax.axis_index("group"), lax.axis_index("tensor")
    planes = groups // pair
    z, x = lax.div(me, pair), lax.rem(me, pair)
    partner = z * pair + 1 - x
    cached, prefix, _ = k_ref.shape
    units, _, width = q_ref.shape
    wide = width // pair
    per_kv = wide // HEAD
    turns = cos_ref.shape[0]
    held = units // turns
    share = turns // lanes
    full_pair, full_plane = full
    factor = math.log2(math.e) / math.sqrt(HEAD)
    wide_a = r_in_a.shape[-1]
    wide_b = wide - wide_a
    send_row, comp_row, ret_row, slot_row = 3, 3 + planes, 3 + 2 * planes, 3 + 3 * planes

    barrier = pltpu.get_barrier_semaphore()

    def greet(step, carry):
        pl.semaphore_signal(
            barrier, inc=1, device_id=(lax.rem(me + step, groups), lane), device_id_type=MESH
        )
        return carry

    lax.fori_loop(1, groups, greet, 0)
    for turn in range(1, lanes):
        for j in range(pair):
            pl.semaphore_signal(
                barrier, inc=1,
                device_id=(z * pair + j, lax.rem(lane + turn, lanes)), device_id_type=MESH,
            )

    def span_of(j):
        return pl.ds(pl.multiple_of(j * HEAD, HEAD), HEAD)

    own = [
        pltpu.make_async_copy(
            ref.at[:, :, span_of(x)], full_ref.at[pl.ds(x * cached, cached)], kv_here.at[i]
        )
        for i, (ref, full_ref) in enumerate(((k_ref, k_all), (v_ref, v_all)))
    ]
    for copy in own:
        copy.start()

    def remote(src, dst, send_sem, recv_sem, group, to_lane):
        return pltpu.make_async_remote_copy(
            src_ref=src, dst_ref=dst, send_sem=send_sem, recv_sem=recv_sem,
            device_id=(group, to_lane), device_id_type=MESH,
        )

    def kv_copies(half):
        return [
            remote(
                ref.at[:, :, span_of(1 - x)], full_ref.at[pl.ds(half * cached, cached)],
                kv_send.at[i], kv_recv.at[i], partner, lane,
            )
            for i, (ref, full_ref) in enumerate(((k_ref, k_all), (v_ref, v_all)))
        ]

    def q_copy(plane, j, source, device):
        return remote(
            q_out.at[plane, j], q_in.at[source], q_send.at[plane, j], q_recv.at[source],
            device, lane,
        )

    def fill(plane):
        def one(k, carry):
            index = tables[send_row + plane, k]
            turn = lax.rem(index, turns)
            cos, sin = cos_ref[turn], sin_ref[turn]
            block = q_ref[index].astype(jnp.float32)
            for j in range(pair):
                parts = []
                for g in range(per_kv):
                    head = j * per_kv + g
                    part = block[:, head * HEAD:(head + 1) * HEAD]
                    turned = part * cos + pltpu.roll(part, HEAD // 2, 1) * sin
                    parts.append(turned.astype(jnp.bfloat16))
                q_out[plane, j, k] = jnp.concatenate(parts, axis=1)
            return carry

        lax.fori_loop(0, cap1, one, 0, unroll=2)

    def dispatch(step, carry):
        plane = xor_order(step, z, planes)
        fill(plane)

        @pl.when(step == 0)
        def _():
            pl.semaphore_wait(barrier, groups - 1 + pair * (lanes - 1))

        for j in range(pair):
            @pl.when((step < planes - 1) | (j != x))
            def _():
                q_copy(plane, j, me, plane * pair + j).start()
        return carry

    lax.fori_loop(0, planes, dispatch, 0)
    for copy in kv_copies(x):
        copy.start()
    q_in[me] = q_out[z, x]
    for copy in own:
        copy.wait()

    def arrive(step, carry):
        other = lax.rem(me + step, groups)
        q_copy(z, x, other, other).wait_recv()
        return carry

    lax.fori_loop(1, groups, arrive, 0)
    for copy in kv_copies(1 - x):
        copy.wait_recv()

    def ra_copy(plane, at, device):
        return remote(
            r_out_a.at[plane], r_in_a.at[at], ra_send.at[plane], ra_recv.at[at], device, lane
        )

    def rb_copy(plane, at, device):
        return remote(
            r_out_b.at[plane], r_in_b.at[at], rb_send.at[plane], rb_recv.at[at], device, lane
        )

    def work(step, carry):
        plane = xor_order(step, z, planes)

        def batch(b, inner):
            slot = tables[slot_row + plane, b]
            blocks = []
            for i in range(BATCH):
                index = tables[comp_row + plane, b * BATCH + i]
                source = plane * pair + lax.div(index, full_pair)
                blocks.append(q_in[source, lax.rem(index, full_pair)].astype(jnp.float32))
            query = jnp.concatenate(
                [block[:, g * HEAD:(g + 1) * HEAD] for g in range(per_kv) for block in blocks],
                axis=0,
            ).astype(jnp.bfloat16)
            scores = lax.dot_general(
                query, k_all[slot], (((1,), (1,)), ((), ())), preferred_element_type=jnp.float32
            )
            peak = jnp.max(scores, axis=-1, keepdims=True)
            weight = jnp.exp2((scores - peak) * factor)
            total = jnp.sum(weight, axis=-1, keepdims=True)
            mixed = jnp.dot(
                weight.astype(jnp.bfloat16), v_all[slot], preferred_element_type=jnp.float32
            ) / total
            for i in range(BATCH):
                results[b * BATCH + i] = jnp.concatenate(
                    [
                        mixed[(g * BATCH + i) * UNIT:(g * BATCH + i + 1) * UNIT]
                        for g in range(per_kv)
                    ],
                    axis=1,
                ).astype(jnp.bfloat16)
            return inner

        lax.fori_loop(0, batches, batch, 0)

        def pack(k, inner):
            found = results[tables[ret_row + plane, k]]
            r_out_a[plane, k] = found[:, :wide_a]
            r_out_b[plane, k] = found[:, wide_a:]
            return inner

        lax.fori_loop(0, cap2, pack, 0, unroll=2)

        @pl.when(step < planes - 1)
        def _():
            ra_copy(plane, z, plane * pair + x).start()
        return carry

    lax.fori_loop(0, planes, work, 0)

    def second(step, carry):
        plane = xor_order(step, z, planes)
        rb_copy(plane, z, plane * pair + x).start()
        return carry

    lax.fori_loop(0, planes - 1, second, 0)
    r_in_a[z] = r_out_a[z]
    r_in_b[z] = r_out_b[z]

    start_of = (lane * pair + x) * wide

    def finish(r_copy, r_in, stage, f_send, f_recv, skip, part):
        def back(step, carry):
            plane = xor_order(step, z, planes)
            r_copy(plane, plane, plane * pair + x).wait_recv()
            return carry

        lax.fori_loop(0, planes - 1, back, 0)

        def spread(step, carry):
            to_lane = lax.rem(lane + lax.div(step + 1, pair), lanes)
            to_x = lax.rem(x + step + 1, pair)

            def one(i, inner):
                item = (z * pair + to_x) * held + i
                entry = tables[2, item]
                length = lax.rem(tables[1, item], LANES)
                source, rank = lax.div(entry, full_plane), lax.rem(entry, full_plane)
                for s in range(share):
                    unit = to_lane * share + s
                    found = r_in[source, jnp.minimum(rank + unit, cap2 - 1)].astype(jnp.float32)
                    row = unit * UNIT + lax.broadcasted_iota(jnp.int32, found.shape, 0)
                    stage[to_x, to_lane, i * share + s] = jnp.where(
                        row < length, found, 0.0
                    ).astype(jnp.bfloat16)
                return inner

            lax.fori_loop(0, held, one, 0, unroll=2)

            @pl.when(step < pair * lanes - 1)
            def _():
                final(to_x, to_lane, x, lane, to_x, to_lane).start()
            return carry

        def final(at_x, at_lane, from_x, from_lane, to_x, to_lane):
            start = pl.multiple_of((from_lane * pair + from_x) * wide + skip, HEAD)
            return remote(
                stage.at[at_x, at_lane], out_ref.at[:, :, pl.ds(start, part)],
                f_send.at[at_x, at_lane], f_recv.at[from_x, from_lane],
                z * pair + to_x, to_lane,
            )

        lax.fori_loop(0, pair * lanes, spread, 0)
        start = pl.multiple_of(start_of + skip, HEAD)
        out_ref[:, :, pl.ds(start, part)] = stage[x, lane]
        return final

    final_a = finish(ra_copy, r_in_a, stage_a, fa_send, fa_recv, 0, wide_a)
    final_b = finish(rb_copy, r_in_b, stage_b, fb_send, fb_recv, wide_a, wide_b)

    def drain(step, carry):
        to_lane = lax.rem(lane + lax.div(step + 1, pair), lanes)
        to_x = lax.rem(x + step + 1, pair)
        for final in (final_a, final_b):
            final(to_x, to_lane, to_x, to_lane, to_x, to_lane).wait_recv()
            final(to_x, to_lane, x, lane, to_x, to_lane).wait_send()
        return carry

    lax.fori_loop(0, pair * lanes - 1, drain, 0)

    def settle(step, carry):
        plane = xor_order(step, z, planes)
        for j in range(pair):
            @pl.when((step < planes - 1) | (j != x))
            def _():
                q_copy(plane, j, me, plane * pair + j).wait_send()

        @pl.when(step < planes - 1)
        def _():
            ra_copy(plane, z, plane * pair + x).wait_send()
            rb_copy(plane, z, plane * pair + x).wait_send()
        return carry

    lax.fori_loop(0, planes, settle, 0)
    for copy in kv_copies(x):
        copy.wait_send()


def packed(groups, lanes, queries, prefix_keys, prefix_values, slot_of_prompt, prompt_of, lengths):
    held, rows, width = queries.shape
    cached, prefix, kv_width = prefix_keys.shape
    pair = kv_width // HEAD
    planes = groups // pair
    turns = rows // UNIT
    full_pair = CAPC * pair * turns
    full_plane = full_pair * pair
    slots = cached * pair
    share = turns // lanes
    wide = width // pair
    per_kv = wide // HEAD
    wide_a = (per_kv + 1) // 2 * HEAD
    wide_b = wide - wide_a
    levels = [
        (math.ceil(full_pair * one), math.ceil(full_plane * two)) for one, two in LEVELS
    ]
    batch_caps = [(cap2 + slots * (BATCH - 1)) // BATCH for _, cap2 in levels]
    smem = pl.BlockSpec(memory_space=pltpu.SMEM)
    vmem = pl.BlockSpec(memory_space=pltpu.VMEM)
    dma = pltpu.SemaphoreType.DMA
    bf16 = jnp.bfloat16
    table_rows = -(-(3 + 4 * planes) // 8) * 8
    full = (full_pair, full_plane)
    tables = pl.pallas_call(
        functools.partial(plan_kernel, groups, pair, levels, full, batch_caps),
        out_shape=jax.ShapeDtypeStruct((table_rows, LANES), jnp.int32),
        in_specs=[smem] * 3,
        out_specs=vmem,
        scratch_shapes=[
            pltpu.VMEM((1, LANES), jnp.int32),
            pltpu.VMEM((groups, 1, LANES), jnp.int32),
            dma((groups,)), dma((groups,)),
        ],
        compiler_params=pltpu.CompilerParams(collective_id=1, has_side_effects=True),
        name="routing_tables",
    )(slot_of_prompt, prompt_of, lengths)

    cos, sin = rotary_tables(prefix, rows)
    shaped = (turns, UNIT, HEAD)
    operands = (
        tables, queries.reshape(held * turns, UNIT, width), prefix_keys, prefix_values,
        jnp.asarray(cos.reshape(shaped)), jnp.asarray(sin.reshape(shaped)),
    )

    def branch(level):
        cap1, cap2 = levels[level]
        batches = batch_caps[level]

        def run(*values):
            return pl.pallas_call(
                functools.partial(packed_kernel, groups, lanes, pair, full, cap1, cap2, batches),
                out_shape=jax.ShapeDtypeStruct((held * share, UNIT, width * lanes), bf16),
                in_specs=[smem] + [vmem] * 5,
                out_specs=vmem,
                scratch_shapes=[
                    pltpu.VMEM((planes, pair, cap1, UNIT, wide), bf16),
                    pltpu.VMEM((groups, cap1, UNIT, wide), bf16),
                    pltpu.VMEM((slots, prefix, HEAD), bf16),
                    pltpu.VMEM((slots, prefix, HEAD), bf16),
                    pltpu.VMEM((batches * BATCH, UNIT, wide), bf16),
                    pltpu.VMEM((planes, cap2, UNIT, wide_a), bf16),
                    pltpu.VMEM((planes, cap2, UNIT, wide_b), bf16),
                    pltpu.VMEM((planes, cap2, UNIT, wide_a), bf16),
                    pltpu.VMEM((planes, cap2, UNIT, wide_b), bf16),
                    pltpu.VMEM((pair, lanes, held * share, UNIT, wide_a), bf16),
                    pltpu.VMEM((pair, lanes, held * share, UNIT, wide_b), bf16),
                    dma((planes, pair)), dma((groups,)), dma((2,)), dma((2,)), dma((2,)),
                    dma((planes,)), dma((planes,)), dma((planes,)), dma((planes,)),
                    dma((pair, lanes)), dma((pair, lanes)),
                    dma((pair, lanes)), dma((pair, lanes)),
                ],
                compiler_params=pltpu.CompilerParams(
                    collective_id=2 + level, has_side_effects=True
                ),
                name=f"packed_prefix_attention_{level}",
            )(*values)

        return run

    out = lax.switch(tables[0, 0], [branch(level) for level in range(len(levels))], *operands)
    return out.reshape(held, share * UNIT, width * lanes)


def fits(groups, lanes, queries, prefix_keys):
    held, rows, width = queries.shape
    pair = prefix_keys.shape[2] // HEAD
    if pair != 2 or groups % (2 * pair) or rows % (UNIT * lanes):
        return False
    planes = groups // pair
    spots = planes * planes * pair * prefix_keys.shape[0]
    full_plane = CAPC * pair * pair * rows // UNIT
    room = full_plane + pair * prefix_keys.shape[0] * (BATCH - 1)
    return groups * held <= LANES and spots <= LANES and room <= LANES


def local(groups, lanes, queries, prefix_keys, *rest):
    form = packed if fits(groups, lanes, queries, prefix_keys) else padded
    return form(groups, lanes, queries, prefix_keys, *rest)


def solution(mesh):
    placed = (
        P("group", None, "tensor"),
        P("group", None, "tensor"),
        P("group", None, "tensor"),
        P(),
        P("group"),
        P("group"),
    )
    return jax.shard_map(
        functools.partial(local, mesh.shape["group"], mesh.shape["tensor"]),
        mesh=mesh, in_specs=placed, out_specs=P("group", "tensor", None), check_vma=False,
    )
```

```python
import functools
import math

import numpy as np

import jax
import jax.numpy as jnp
from jax import lax
from jax.experimental import pallas as pl
from jax.experimental.pallas import tpu as pltpu
from jax.sharding import PartitionSpec as P

HEAD = 128
CAPC = 2
ROTARY_BASE = 1000000.0
TILE = 16
UNIT = 8
BATCH = 4
LANES = 128
MESH = pl.DeviceIdType.MESH
PIECES = 3
LEVELS = (
    (0.65625, 0.453125, 0.65625, 0.5625),
    (0.65625, 0.515625, 0.65625, 0.5625),
    (0.75, 0.515625, 0.75, 0.625),
    (0.75, 0.578125, 0.875, 0.6875),
    (0.875, 0.6875, 1, 0.78125),
    (1, 1, 1, 1),
)


def rotary_tables(first_position, rows):
    half = HEAD // 2
    frequencies = np.float32(ROTARY_BASE) ** (
        -(np.arange(half, dtype=np.float32) * np.float32(2.0) / np.float32(HEAD))
    )
    positions = (first_position + np.arange(rows)).astype(np.float32)
    angles = (positions[:, None] * frequencies.astype(np.float32)[None, :]).astype(np.float64)
    cos, sin = np.cos(angles), np.sin(angles)
    return (
        np.concatenate([cos, cos], axis=1).astype(np.float32),
        np.concatenate([-sin, sin], axis=1).astype(np.float32),
    )


def padded_kernel(
    groups, lanes, moved,
    source_ref, tag_ref, dest_ref, length_ref,
    q_ref, k_ref, v_ref, cos_ref, sin_ref,
    out_ref,
    q_out, q_in, sel_out, sel_in, res, stage,
    q_send, q_recv, s_send, s_recv, r_send, r_recv,
    *near,
):
    me, lane = lax.axis_index("group"), lax.axis_index("tensor")
    held, rows, width = q_ref.shape
    cached, prefix, kv_width = k_ref.shape
    share = rows // lanes
    kv_local = kv_width // HEAD
    per_kv = width // HEAD // kv_local
    half = groups // 2
    factor = math.log2(math.e) / math.sqrt(HEAD)
    wide_near = moved * per_kv * HEAD
    if moved:
        (n_out, n_in, ns_out, ns_in, n_res, k_far, v_far,
         n_send, n_recv, ns_send, ns_recv, nr_send, nr_recv, kv_send, kv_recv) = near
    spot = lax.rem(me, half)
    base = me - spot
    mirror = lax.rem(me + half, groups)

    barrier = pltpu.get_barrier_semaphore()

    def greet(step, carry):
        for turn in range(lanes):
            def send():
                pl.semaphore_signal(
                    barrier, inc=1,
                    device_id=(lax.rem(me + step, groups), lax.rem(lane + turn, lanes)),
                    device_id_type=MESH,
                )
            if turn:
                send()
            else:
                pl.when(step > 0)(send)
        return carry

    lax.fori_loop(0, groups, greet, 0)

    def offset_of(step):
        swing = (step + 1) // 2
        return lax.rem(half + (1 - 2 * lax.rem(step, 2)) * swing + groups, groups)

    def route(owner):
        places = [owner * CAPC + slot for slot in range(CAPC)]
        return [(source_ref[place], tag_ref[place]) for place in places]

    def fill(items, q_to, sel_to, block, first, last):
        for slot, (item, tag) in enumerate(items):
            for j in range(cached):
                weight = jnp.where(tag == j, 1.0, 0.0)
                sel_to[block, slot * cached + j] = jnp.full(
                    (TILE, HEAD), weight, jnp.float32
                ).astype(jnp.bfloat16)
            for head in range(first, last):
                x = q_ref[item, :, head * HEAD:(head + 1) * HEAD].astype(jnp.float32)
                turned = x * cos_ref[...] + pltpu.roll(x, HEAD // 2, 1) * sin_ref[...]
                span = slice((head - first) * HEAD, (head - first + 1) * HEAD)
                q_to[block, slot, :, span] = turned.astype(jnp.bfloat16)

    near_heads, all_heads = moved * per_kv, width // HEAD

    def pair(src, dst, send_sem, recv_sem, device):
        return pltpu.make_async_remote_copy(
            src_ref=src, dst_ref=dst, send_sem=send_sem, recv_sem=recv_sem,
            device_id=device, device_id_type=MESH,
        )

    def q_copies(here, there, device):
        return (
            pair(sel_out.at[here], sel_in.at[there], s_send.at[here], s_recv.at[there],
                 (device, lane)),
            pair(q_out.at[here], q_in.at[there], q_send.at[here], q_recv.at[there],
                 (device, lane)),
        )

    def n_copies(here, there, device):
        return (
            pair(ns_out.at[here], ns_in.at[there], ns_send.at[here], ns_recv.at[there],
                 (device, lane)),
            pair(n_out.at[here], n_in.at[there], n_send.at[here], n_recv.at[there],
                 (device, lane)),
        )

    def place(owner, from_lane, skip, wide):
        start = pl.multiple_of(from_lane * width + skip, HEAD)
        return stage.at[pl.ds(owner * CAPC, CAPC), :, pl.ds(start, wide)]

    def r_copy(block, piece, owner, from_lane, device):
        return pair(
            res.at[block, :, piece], place(owner, from_lane, wide_near, width - wide_near),
            r_send.at[block, piece], r_recv.at[owner, from_lane], (device, piece),
        )

    def nr_copy(block, piece, owner, from_lane, device):
        return pair(
            n_res.at[block, :, piece], place(owner, from_lane, 0, wide_near),
            nr_send.at[block, piece], nr_recv.at[owner, from_lane], (device, piece),
        )

    def kv_copies():
        span = pl.ds(0, moved * HEAD)
        return (
            pair(k_ref.at[:, :, span], k_far, kv_send.at[0], kv_recv.at[0], (mirror, lane)),
            pair(v_ref.at[:, :, span], v_far, kv_send.at[1], kv_recv.at[1], (mirror, lane)),
        )

    items = route(mirror)
    fill(items, q_out, sel_out, mirror, near_heads, all_heads)
    pl.semaphore_wait(barrier, groups * lanes - 1)
    for copy in q_copies(mirror, me, mirror):
        copy.start()
    if moved:
        fill(items, n_in, ns_in, spot + half, 0, near_heads)

    def dispatch(step, carry):
        owner = lax.rem(me + offset_of(step), groups)
        items = route(owner)
        fill(items, q_out, sel_out, owner, near_heads, all_heads)
        for copy in q_copies(owner, me, owner):
            copy.start()
        if moved:
            fill(items, n_out, ns_out, owner, 0, near_heads)
            seat = lax.rem(owner, half)
            kind = lax.rem(lax.div(owner, half) + lax.div(me, half), 2)
            for copy in n_copies(owner, spot + half * kind, base + seat):
                copy.start()
        return carry

    lax.fori_loop(1, groups - 1, dispatch, 0)
    if moved:
        for copy in kv_copies():
            copy.start()
    items = route(me)
    fill(items, q_in, sel_in, me, near_heads, all_heads)
    if moved:
        fill(items, n_in, ns_in, spot, 0, near_heads)

    def attend(q_from, sel_from, to, block, keys, values, first, count):
        for slot in range(CAPC):
            weights = [sel_from[block, slot * cached + j][None] for j in range(cached)]

            def chosen(ref, span):
                total = None
                for j in range(cached):
                    part = ref[j, :, span].reshape(prefix // TILE, TILE, HEAD) * weights[j]
                    total = part if total is None else total + part
                return total.reshape(prefix, HEAD)

            for kv in range(count):
                span = slice((first + kv) * HEAD, (first + kv + 1) * HEAD)
                spans = [
                    slice((kv * per_kv + g) * HEAD, (kv * per_kv + g + 1) * HEAD)
                    for g in range(per_kv)
                ]
                query = jnp.concatenate([q_from[block, slot, :, s] for s in spans], axis=0)
                scores = lax.dot_general(
                    query, chosen(keys, span), (((1,), (1,)), ((), ())),
                    preferred_element_type=jnp.float32,
                )
                peak = jnp.max(scores, axis=-1, keepdims=True)
                weight = jnp.exp2((scores - peak) * factor)
                total = jnp.sum(weight, axis=-1, keepdims=True)
                mixed = jnp.dot(
                    weight.astype(jnp.bfloat16), chosen(values, span),
                    preferred_element_type=jnp.float32,
                )
                mixed = (mixed / total).astype(jnp.bfloat16)
                for g in range(per_kv):
                    to[block, slot, :, :, spans[g]] = mixed[g * rows:(g + 1) * rows].reshape(
                        lanes, share, HEAD
                    )

    def give_back(step, copy, source, block, owner, done, skip, wide):
        for turn in range(1, lanes):
            copy(block, lax.rem(lane + turn, lanes), owner, lane, source).start()

        @pl.when(step > 0)
        def _():
            copy(block, lane, owner, lane, source).start()

        @pl.when(step == 0)
        def _():
            start = pl.multiple_of(lane * width + skip, HEAD)
            stage[pl.ds(owner * CAPC, CAPC), :, pl.ds(start, wide)] = done[block, :, lane]

    def far_work(step, carry):
        source = lax.rem(me + groups - offset_of(lax.rem(step + groups - 1, groups)), groups)

        @pl.when(step > 0)
        def _():
            for copy in q_copies(source, source, source):
                copy.wait_recv()

        attend(q_in, sel_in, res, source, k_ref, v_ref, moved, kv_local - moved)
        give_back(step, r_copy, source, source, me, res, wide_near, width - wide_near)
        return carry

    def near_work(kind, keys, values, owner):
        def body(step, carry):
            seat = lax.rem(spot + step, half)
            block = seat + half * kind

            @pl.when(step > 0)
            def _():
                for copy in n_copies(block, block, base + seat):
                    copy.wait_recv()

            attend(n_in, ns_in, n_res, block, keys, values, 0, moved)
            give_back(step, nr_copy, base + seat, block, owner, n_res, 0, wide_near)
            return carry

        lax.fori_loop(0, half, body, 0)

    if moved:
        near_work(0, k_ref, v_ref, me)
    lax.fori_loop(0, groups, far_work, 0)
    if moved:
        for copy in kv_copies():
            copy.wait_recv()
        near_work(1, k_far, v_far, mirror)

    def returned(step, copy, block, owner, device):
        @pl.when(step > 0)
        def _():
            copy(block, lane, owner, lane, device).wait_send()
            copy(block, lane, owner, lane, device).wait_recv()

        for turn in range(1, lanes):
            piece = lax.rem(lane + turn, lanes)
            copy(block, piece, owner, piece, device).wait_send()
            copy(block, piece, owner, piece, device).wait_recv()

    def far_settle(step, carry):
        other = lax.rem(me + step, groups)

        @pl.when(step > 0)
        def _():
            for copy in q_copies(other, me, other):
                copy.wait_send()

        returned(step, r_copy, other, other, other)
        return carry

    lax.fori_loop(0, groups, far_settle, 0)
    if moved:
        for copy in kv_copies():
            copy.wait_send()

        def near_settle(step, carry):
            seat = lax.rem(spot + step, half)
            for kind in range(2):
                owner = lax.rem(base + half * kind, groups) + seat

                @pl.when(step > 0)
                def _():
                    for copy in n_copies(owner, owner, base + seat):
                        copy.wait_send()

                returned(step, nr_copy, seat + half * kind, owner, base + seat)
            return carry

        lax.fori_loop(0, half, near_settle, 0)

    def deliver(item, carry):
        found = stage[dest_ref[item]].astype(jnp.float32)
        position = lane * share + lax.broadcasted_iota(jnp.int32, found.shape, 0)
        out_ref[item] = jnp.where(position < length_ref[item], found, 0.0).astype(jnp.bfloat16)
        return carry

    lax.fori_loop(0, held, deliver, 0)


def padded(groups, lanes, queries, prefix_keys, prefix_values, slot_of_prompt, prompt_of, lengths):
    held, rows, width = queries.shape
    cached, prefix, kv_width = prefix_keys.shape
    share = rows // lanes
    kv_local = kv_width // HEAD
    moved = kv_local // 2 if groups % 2 == 0 and groups >= 4 else 0
    wide_near = moved * (width // kv_local)
    wide = width - wide_near
    cos, sin = rotary_tables(prefix, rows)
    cache_rows = slot_of_prompt[prompt_of]
    owner = cache_rows // cached
    serial = jnp.arange(held)
    earlier = (owner[None, :] == owner[:, None]) & (serial[None, :] < serial[:, None])
    destination = owner * CAPC + jnp.sum(earlier.astype(jnp.int32), axis=1)
    matches = destination[None, :] == jnp.arange(groups * CAPC)[:, None]
    source = jnp.sum(jnp.where(matches, serial[None, :], 0), axis=1)
    tags = jnp.sum(jnp.where(matches, (cache_rows % cached)[None, :], 0), axis=1)
    smem = pl.BlockSpec(memory_space=pltpu.SMEM)
    vmem = pl.BlockSpec(memory_space=pltpu.VMEM)
    dma = pltpu.SemaphoreType.DMA
    bf16 = jnp.bfloat16

    def exchange(features):
        return [
            pltpu.VMEM((groups, CAPC, rows, features), bf16),
            pltpu.VMEM((groups, CAPC, rows, features), bf16),
            pltpu.VMEM((groups, CAPC * cached, TILE, HEAD), bf16),
            pltpu.VMEM((groups, CAPC * cached, TILE, HEAD), bf16),
            pltpu.VMEM((groups, CAPC, lanes, share, features), bf16),
        ]

    semaphores = [
        dma((groups,)), dma((groups,)),
        dma((groups,)), dma((groups,)),
        dma((groups, lanes)), dma((groups, lanes)),
    ]
    scratch = [
        *exchange(wide),
        pltpu.VMEM((groups * CAPC, share, width * lanes), bf16),
        *semaphores,
    ]
    if moved:
        scratch += [
            *exchange(wide_near),
            pltpu.VMEM((cached, prefix, moved * HEAD), bf16),
            pltpu.VMEM((cached, prefix, moved * HEAD), bf16),
            *semaphores,
            dma((2,)), dma((2,)),
        ]
    return pl.pallas_call(
        functools.partial(padded_kernel, groups, lanes, moved),
        out_shape=jax.ShapeDtypeStruct((held, share, width * lanes), bf16),
        in_specs=[smem] * 4 + [vmem] * 5,
        out_specs=vmem,
        scratch_shapes=scratch,
        compiler_params=pltpu.CompilerParams(collective_id=0, has_side_effects=True),
        name="routed_prefix_attention",
    )(
        source.astype(jnp.int32), tags.astype(jnp.int32), destination.astype(jnp.int32), lengths,
        queries, prefix_keys, prefix_values, jnp.asarray(cos), jnp.asarray(sin),
    )


def xor_order(step, plane, planes):
    half = planes // 2
    near = lax.div(step, half)
    side = lax.rem(lax.div(plane, half) + 1 - near, 2)
    return side * half + lax.rem(lax.rem(plane, half) + step + near, half)


def step_of(plane, z, planes):
    half = planes // 2
    shift = lax.rem(plane + planes - z, half)
    far = shift
    near = half + lax.rem(shift + half - 1, half)
    return jnp.where(plane // half != z // half, far, near)


def plan_kernel(
    groups, pair, levels, full, base,
    slot_ref, prompt_ref, length_ref, q_ref, k_ref, v_ref, cos_ref, sin_ref,
    tables_ref, level_ref, k_far, v_far, q_base,
    mine, gathered, q_out, send, recv, q_send, q_recv, kv_send, kv_recv,
):
    shared = len(base)
    me, lane = lax.axis_index("group"), lax.axis_index("tensor")
    held = prompt_ref.shape[0]
    slots = slot_ref.shape[0]
    planes = groups // pair
    per_plane = slots // planes
    total = groups * held
    full_pair, full_plane = full
    turns = full_pair // (CAPC * pair)
    half = planes // 2
    z, x = lax.div(me, pair), lax.rem(me, pair)
    partner = z * pair + 1 - x
    there = [xor_order(step, z, planes) for step in range(shared)]
    barrier = pltpu.get_barrier_semaphore()

    def greet(step, carry):
        pl.semaphore_signal(
            barrier, inc=1, device_id=(lax.rem(me + step, groups), lane), device_id_type=MESH
        )
        return carry

    lax.fori_loop(1, groups, greet, 0)

    def remote(src, dst, send_sem, recv_sem, group):
        return pltpu.make_async_remote_copy(
            src_ref=src, dst_ref=dst, send_sem=send_sem, recv_sem=recv_sem,
            device_id=(group, lane), device_id_type=MESH,
        )

    span = pl.ds(pl.multiple_of((1 - x) * HEAD, HEAD), HEAD)
    kv_copies = [
        remote(ref.at[:, :, span], far_ref, kv_send.at[i], kv_recv.at[i], partner)
        for i, (ref, far_ref) in enumerate(((k_ref, k_far), (v_ref, v_far)))
    ]

    def q_copy(step, j, source, device):
        return remote(
            q_out.at[step, j, pl.ds(0, base[step])], q_base.at[step, source, pl.ds(0, base[step])],
            q_send.at[step, j], q_recv.at[step, source], device,
        )

    own_slots = [slot_ref[prompt_ref[i]] for i in range(held)]
    own_planes = [lax.div(slot, per_plane) for slot in own_slots]
    own_counts = [lax.div(length_ref[i] + UNIT - 1, UNIT) for i in range(held)]
    own_starts = []
    for i in range(held):
        start = jnp.int32(0)
        for other in range(i):
            start = start + jnp.where(own_planes[other] == own_planes[i], own_counts[other], 0)
        own_starts.append(start)

    def fill(step):
        starts = [
            jnp.where(own_planes[i] == there[step], own_starts[i], LANES) for i in range(held)
        ]

        def one(k, carry):
            index = jnp.int32(0)
            for i in range(held):
                offset = k - starts[i]
                hit = (offset >= 0) & (offset < own_counts[i])
                index = index + jnp.where(hit, i * turns + offset, 0)
            rope(index, q_ref, cos_ref, sin_ref, q_out.at[step], k, pair)
            return carry

        lax.fori_loop(0, base[step], one, 0)

    lanes1 = lax.broadcasted_iota(jnp.int32, (1, LANES), 1)
    row = jnp.zeros((1, LANES), jnp.int32)
    for i in range(held):
        value = own_slots[i] * LANES + length_ref[i]
        row = jnp.where(lanes1 == me * held + i, value, row)
    mine[...] = row
    gathered[me] = row
    for step in range(half):
        fill(step)
    pl.semaphore_wait(barrier, groups - 1)

    def copy(there, device):
        return pltpu.make_async_remote_copy(
            src_ref=mine, dst_ref=gathered.at[there], send_sem=send.at[device],
            recv_sem=recv.at[there], device_id=(device, lane), device_id_type=MESH,
        )

    def push(step, carry):
        copy(me, lax.rem(me + step, groups)).start()
        return carry

    lax.fori_loop(1, groups, push, 0)

    def dispatch(step):
        for j in range(pair):
            q_copy(step, j, x, there[step] * pair + j).start()

    for step in range(half):
        dispatch(step)
    for kv_copy in kv_copies:
        kv_copy.start()
    for step in range(half, shared):
        fill(step)
        dispatch(step)

    def settle(step, carry):
        other = lax.rem(me + step, groups)
        copy(other, other).wait_recv()
        copy(me, other).wait_send()
        return carry

    lax.fori_loop(1, groups, settle, 0)
    code = gathered[0]
    for g in range(1, groups):
        code = code + gathered[g]

    square = (LANES, LANES)
    down = lax.broadcasted_iota(jnp.int32, square, 0)
    across = lax.broadcasted_iota(jnp.int32, square, 1)
    eye = down == across

    def to_column(values):
        return jnp.sum(jnp.where(eye, jnp.broadcast_to(values, square), 0), axis=1, keepdims=True)

    def to_row(values):
        return jnp.sum(jnp.where(eye, jnp.broadcast_to(values, square), 0), axis=0, keepdims=True)

    def facts(values, index):
        live = index < total
        length = values % LANES
        slot = values // LANES
        count = jnp.where(live, (length + UNIT - 1) // UNIT, 0)
        return count, slot, slot // per_plane, index // held, index // (held * pair)

    col = to_column(code)
    down1 = lax.broadcasted_iota(jnp.int32, (LANES, 1), 0)
    count_r, slot_r, to_r, from_r, plane_r = facts(code, lanes1)
    count_c, slot_c, to_c, from_c, plane_c = facts(col, down1)
    weight = jnp.broadcast_to(count_c, square)
    earlier = (down < across) & (to_c == to_r)

    def rank(mask):
        return jnp.sum(jnp.where(mask, weight, 0), axis=0, keepdims=True)

    base1 = rank(earlier & (from_c == from_r))
    base2 = rank(earlier & (plane_c == plane_r))
    within = rank(earlier & (plane_c == plane_r) & (slot_c == slot_r))
    key_r = plane_r * slots + slot_r
    number = jnp.sum(
        jnp.where(down1 == key_r, jnp.broadcast_to(count_r, square), 0), axis=1, keepdims=True
    )
    need = (number + BATCH - 1) // BATCH
    need_r = to_row(need)
    first = jnp.sum(
        jnp.where(
            (down // per_plane == across // per_plane) & (across < down),
            jnp.broadcast_to(need_r, square), 0,
        ),
        axis=1, keepdims=True,
    )
    first_of = jnp.sum(
        jnp.where(down1 == key_r, jnp.broadcast_to(first, square), 0), axis=0, keepdims=True
    )
    place = first_of * BATCH + within
    base1_c, base2_c, place_c = to_column(base1), to_column(base2), to_column(place)

    alive = lanes1 < total
    far = alive & (to_r // half != plane_r // half)
    near = alive & (to_r // half == plane_r // half)
    needs = [
        jnp.max(jnp.where(mask, base + count_r, 0))
        for mask in (far, near) for base in (base1, base2)
    ]
    level = jnp.int32(len(levels) - 1)
    for index, caps in reversed(list(enumerate(levels[:-1]))):
        over = needs[0] > caps[0]
        for value, cap in zip(needs[1:], caps[1:]):
            over = over | (value > cap)
        level = jnp.where(over, level, index)
    level_ref[0] = level
    tables_ref[pl.ds(1, 1), :] = code
    tables_ref[pl.ds(2, 1), :] = step_of(to_r, z, planes) * full_plane + base2

    def pick(mask, start_c, value_c, index):
        hit = mask & (index >= start_c) & (index < start_c + count_c)
        return jnp.sum(jnp.where(hit, value_c + index, 0), axis=0, keepdims=True)

    for plane in range(planes):
        tables_ref[pl.ds(3 + plane, 1), :] = pick(
            (from_c == me) & (to_c == plane), base1_c,
            lax.rem(down1, held) * turns - base1_c, lanes1,
        )
        here = (plane_c == plane) & (to_c == z)
        tables_ref[pl.ds(3 + planes + plane, 1), :] = pick(
            here, place_c, lax.rem(from_c, pair) * full_pair + base1_c - place_c, lanes1
        )
        tables_ref[pl.ds(3 + 2 * planes + plane, 1), :] = pick(
            here, base2_c, place_c - base2_c, lanes1
        )
        starts = (
            (down1 // slots == plane) & (lax.rem(down1, slots) // per_plane == z)
            & (lanes1 >= first) & (lanes1 < first + need)
        )
        tables_ref[pl.ds(3 + 3 * planes + plane, 1), :] = jnp.sum(
            jnp.where(starts, lax.rem(down1, per_plane), 0), axis=0, keepdims=True
        )
    for step in range(shared):
        for j in range(pair):
            q_copy(step, j, j, me).wait_recv()
            q_copy(step, j, x, there[step] * pair + j).wait_send()
    for kv_copy in kv_copies:
        kv_copy.wait_recv()
        kv_copy.wait_send()


def rope(index, q_ref, cos_ref, sin_ref, to, k, pair):
    turn = lax.rem(index, cos_ref.shape[0])
    cos, sin = cos_ref[turn], sin_ref[turn]
    block = q_ref[index].astype(jnp.float32)
    per_kv = block.shape[-1] // HEAD // pair
    for j in range(pair):
        parts = []
        for g in range(per_kv):
            head = j * per_kv + g
            part = block[:, head * HEAD:(head + 1) * HEAD]
            turned = part * cos + pltpu.roll(part, HEAD // 2, 1) * sin
            parts.append(turned.astype(jnp.bfloat16))
        to[j, k] = jnp.concatenate(parts, axis=1)


def packed_kernel(
    groups, lanes, pair, full, caps, cuts, base,
    tables,
    q_ref, k_ref, v_ref, k_far, v_far, q_base, cos_ref, sin_ref,
    out_ref,
    *scratch,
):
    me, lane = lax.axis_index("group"), lax.axis_index("tensor")
    planes = groups // pair
    half = planes // 2
    pieces = len(cuts)
    scratch = list(scratch)

    def take(count):
        taken = scratch[:count]
        del scratch[:count]
        return taken

    q_out, q_in, results = take(planes), take(planes), take(planes)
    r_out, r_in, stage = take(pieces), take(pieces), take(pieces)
    k_all, v_all = take(2)
    q_send, q_recv, kv_here, q_here, r_send, r_recv, f_send, f_recv = scratch

    z, x = lax.div(me, pair), lax.rem(me, pair)
    cached, prefix, _ = k_ref.shape
    units, _, width = q_ref.shape
    wide = width // pair
    per_kv = wide // HEAD
    turns = cos_ref.shape[0]
    held = units // turns
    share = turns // lanes
    full_pair, full_plane = full
    cap1, cap2, near1, near2 = caps
    factor = math.log2(math.e) / math.sqrt(HEAD)
    send_row, comp_row, ret_row, slot_row = 3, 3 + planes, 3 + 2 * planes, 3 + 3 * planes
    counts1 = [cap1 if step < half else near1 for step in range(planes)]
    counts2 = [cap2 if step < half else near2 for step in range(planes)]
    offsets = [sum(counts2[:step]) for step in range(planes)]
    last = planes - 1
    there = [xor_order(step, z, planes) for step in range(planes)]

    barrier = pltpu.get_barrier_semaphore()

    def greet(step, carry):
        pl.semaphore_signal(
            barrier, inc=1, device_id=(lax.rem(me + step, groups), lane), device_id_type=MESH
        )
        return carry

    lax.fori_loop(1, groups, greet, 0)
    for turn in range(1, lanes):
        for j in range(pair):
            pl.semaphore_signal(
                barrier, inc=1,
                device_id=(z * pair + j, lax.rem(lane + turn, lanes)), device_id_type=MESH,
            )

    def span_of(j):
        return pl.ds(pl.multiple_of(j * HEAD, HEAD), HEAD)

    here = [
        pltpu.make_async_copy(
            ref.at[:, :, span_of(x)], full_ref.at[pl.ds(x * cached, cached)], kv_here.at[i]
        )
        for i, (ref, full_ref) in enumerate(((k_ref, k_all), (v_ref, v_all)))
    ] + [
        pltpu.make_async_copy(
            far_ref, full_ref.at[pl.ds((1 - x) * cached, cached)], kv_here.at[2 + i]
        )
        for i, (far_ref, full_ref) in enumerate(((k_far, k_all), (v_far, v_all)))
    ] + [
        pltpu.make_async_copy(
            q_base.at[step, :, pl.ds(0, base[step])], q_in[step].at[:, pl.ds(0, base[step])],
            q_here.at[step],
        )
        for step in range(len(base))
    ]
    for copy in here:
        copy.start()

    def remote(src, dst, send_sem, recv_sem, group, to_lane):
        return pltpu.make_async_remote_copy(
            src_ref=src, dst_ref=dst, send_sem=send_sem, recv_sem=recv_sem,
            device_id=(group, to_lane), device_id_type=MESH,
        )

    rest = [
        slice(base[step] if step < len(base) else 0, counts1[step]) for step in range(planes)
    ]

    def q_copy(step, j, source, device):
        span = pl.ds(rest[step].start, rest[step].stop - rest[step].start)
        return remote(
            q_out[step].at[j, span], q_in[step].at[source, span], q_send.at[step, j],
            q_recv.at[step, source], device, lane,
        )

    def fill(step):
        def one(k, carry):
            index = tables[send_row + there[step], k]
            rope(index, q_ref, cos_ref, sin_ref, q_out[step], k, pair)
            return carry

        lax.fori_loop(rest[step].start, rest[step].stop, one, 0)

    moving = [step for step in range(planes) if rest[step].stop > rest[step].start]

    def dispatch(step):
        if step not in moving:
            return
        for j in range(pair):
            if step < last:
                q_copy(step, j, x, there[step] * pair + j).start()
            else:
                @pl.when(j != x)
                def _():
                    q_copy(step, j, x, there[step] * pair + j).start()

    for step in moving:
        fill(step)
    q_in[last][x] = q_out[last][x]

    def greeted():
        pl.semaphore_wait(barrier, groups - 1 + pair * (lanes - 1))
        for step in moving:
            dispatch(step)

    if 0 in moving:
        greeted()
    for copy in here:
        copy.wait()

    def r_copy(piece, step):
        region = pl.ds(offsets[step], counts2[step])
        return remote(
            r_out[piece].at[region], r_in[piece].at[region],
            r_send.at[piece, step], r_recv.at[piece, step], there[step] * pair + x, lane,
        )

    for step in range(planes):
        for j in range(pair) if step in moving else []:
            if step < last:
                q_copy(step, j, j, me).wait_recv()
            else:
                @pl.when(j != x)
                def _():
                    q_copy(step, j, j, me).wait_recv()

        def batch(b, carry):
            slot = tables[slot_row + there[step], b]
            blocks = []
            for i in range(BATCH):
                index = tables[comp_row + there[step], b * BATCH + i]
                blocks.append(
                    q_in[step][lax.div(index, full_pair), lax.rem(index, full_pair)].astype(
                        jnp.float32
                    )
                )
            query = jnp.concatenate(
                [block[:, g * HEAD:(g + 1) * HEAD] for g in range(per_kv) for block in blocks],
                axis=0,
            ).astype(jnp.bfloat16)
            scores = lax.dot_general(
                query, k_all[slot], (((1,), (1,)), ((), ())), preferred_element_type=jnp.float32
            )
            peak = jnp.max(scores, axis=-1, keepdims=True)
            weight = jnp.exp2((scores - peak) * factor)
            total = jnp.sum(weight, axis=-1, keepdims=True)
            mixed = jnp.dot(
                weight.astype(jnp.bfloat16), v_all[slot], preferred_element_type=jnp.float32
            ) / total
            for i in range(BATCH):
                results[step][b * BATCH + i] = jnp.concatenate(
                    [
                        mixed[(g * BATCH + i) * UNIT:(g * BATCH + i + 1) * UNIT]
                        for g in range(per_kv)
                    ],
                    axis=1,
                ).astype(jnp.bfloat16)
            return carry

        lax.fori_loop(0, results[step].shape[0] // BATCH, batch, 0, unroll=2)
        target = r_out if step < last else r_in

        def pack(k, carry):
            found = results[step][tables[ret_row + there[step], k]]
            start = 0
            for piece in range(pieces):
                target[piece][offsets[step] + k] = found[:, start:start + cuts[piece]]
                start += cuts[piece]
            return carry

        lax.fori_loop(0, counts2[step], pack, 0, unroll=2)
        if step == 0 and 0 not in moving:
            greeted()
        if step < last:
            r_copy(0, step).start()
        if step == half - 1 and pieces > 1:
            r_copy(1, 0).start()
        if step == last - 1:
            for piece in range(1, pieces):
                for ready in range(last):
                    if piece > 1 or ready > 0:
                        r_copy(piece, ready).start()

    def lineup(step):
        return lax.rem(x + step + 1, pair), lax.rem(lane + lax.div(step + 1, pair), lanes)

    def final(piece, at_x, at_lane, from_x, from_lane, to_x, to_lane):
        skip = sum(cuts[:piece])
        start = pl.multiple_of((from_lane * pair + from_x) * wide + skip, HEAD)
        return remote(
            stage[piece].at[at_x, at_lane], out_ref.at[:, :, pl.ds(start, cuts[piece])],
            f_send.at[piece, at_x, at_lane], f_recv.at[piece, from_x, from_lane],
            z * pair + to_x, to_lane,
        )

    for piece in range(pieces):
        for step in range(last):
            r_copy(piece, step).wait_recv()

        def spread(step, carry):
            to_x, to_lane = lineup(step)

            def one(i, inner):
                item = (z * pair + to_x) * held + i
                entry = tables[2, item]
                length = lax.rem(tables[1, item], LANES)
                source, rank = lax.div(entry, full_plane), lax.rem(entry, full_plane)
                cap = jnp.where(source < half, cap2, near2)
                offset = jnp.where(
                    source < half, source * cap2, half * cap2 + (source - half) * near2
                )
                for s in range(share):
                    unit = to_lane * share + s
                    found = r_in[piece][offset + jnp.minimum(rank + unit, cap - 1)].astype(
                        jnp.float32
                    )
                    row = unit * UNIT + lax.broadcasted_iota(jnp.int32, found.shape, 0)
                    stage[piece][to_x, to_lane, i * share + s] = jnp.where(
                        row < length, found, 0.0
                    ).astype(jnp.bfloat16)
                return inner

            lax.fori_loop(0, held, one, 0, unroll=2)

            @pl.when(step < pair * lanes - 1)
            def _():
                final(piece, to_x, to_lane, x, lane, to_x, to_lane).start()
            return carry

        lax.fori_loop(0, pair * lanes, spread, 0)
        start = pl.multiple_of((lane * pair + x) * wide + sum(cuts[:piece]), HEAD)
        out_ref[:, :, pl.ds(start, cuts[piece])] = stage[piece][x, lane]

    def drain(step, carry):
        to_x, to_lane = lineup(step)
        for piece in range(pieces):
            final(piece, to_x, to_lane, to_x, to_lane, to_x, to_lane).wait_recv()
            final(piece, to_x, to_lane, x, lane, to_x, to_lane).wait_send()
        return carry

    lax.fori_loop(0, pair * lanes - 1, drain, 0)
    for step in range(planes):
        for j in range(pair) if step in moving else []:
            if step < last:
                q_copy(step, j, x, there[step] * pair + j).wait_send()
            else:
                @pl.when(j != x)
                def _():
                    q_copy(step, j, x, there[step] * pair + j).wait_send()
        if step < last:
            for piece in range(pieces):
                r_copy(piece, step).wait_send()


def packed(groups, lanes, queries, prefix_keys, prefix_values, slot_of_prompt, prompt_of, lengths):
    held, rows, width = queries.shape
    cached, prefix, kv_width = prefix_keys.shape
    pair = kv_width // HEAD
    planes = groups // pair
    half = planes // 2
    turns = rows // UNIT
    full_pair = CAPC * pair * turns
    full_plane = full_pair * pair
    slots = cached * pair
    share = turns // lanes
    wide = width // pair
    per_kv = wide // HEAD
    cuts = [HEAD * (per_kv // PIECES + (i < per_kv % PIECES)) for i in range(PIECES)]
    levels = [
        tuple(math.ceil(full_size * part) for full_size, part in zip((full_pair, full_plane) * 2, level))
        for level in LEVELS
    ]
    smem = pl.BlockSpec(memory_space=pltpu.SMEM)
    vmem = pl.BlockSpec(memory_space=pltpu.VMEM)
    anywhere = pl.BlockSpec(memory_space=pl.ANY)
    dma = pltpu.SemaphoreType.DMA
    bf16 = jnp.bfloat16
    table_rows = -(-(3 + 4 * planes) // 8) * 8
    full = (full_pair, full_plane)
    cos, sin = (jnp.asarray(table.reshape(turns, UNIT, HEAD)) for table in rotary_tables(prefix, rows))
    units = queries.reshape(held * turns, UNIT, width)
    base = [min(level[0] for level in levels)] * half
    base += [min(level[2] for level in levels)] * (planes - half - 1)
    base_shape = (len(base), pair, max(base), UNIT, wide)
    far_shape = jax.ShapeDtypeStruct((cached, prefix, HEAD), bf16)
    tables, chosen, k_far, v_far, q_base = pl.pallas_call(
        functools.partial(plan_kernel, groups, pair, levels, full, base),
        out_shape=[
            jax.ShapeDtypeStruct((table_rows, LANES), jnp.int32),
            jax.ShapeDtypeStruct((1,), jnp.int32),
            far_shape, far_shape,
            jax.ShapeDtypeStruct(base_shape, bf16),
        ],
        in_specs=[smem] * 3 + [vmem, anywhere, anywhere, vmem, vmem],
        out_specs=[vmem, smem] + [anywhere] * 3,
        scratch_shapes=[
            pltpu.VMEM((1, LANES), jnp.int32),
            pltpu.VMEM((groups, 1, LANES), jnp.int32),
            pltpu.VMEM(base_shape, bf16),
            dma((groups,)), dma((groups,)),
            dma((len(base), pair)), dma((len(base), pair)), dma((2,)), dma((2,)),
        ],
        compiler_params=pltpu.CompilerParams(collective_id=1, has_side_effects=True),
        name="plan_and_share",
    )(slot_of_prompt, prompt_of, lengths, units, prefix_keys, prefix_values, cos, sin)
    operands = (tables, units, prefix_keys, prefix_values, k_far, v_far, q_base, cos, sin)

    def branch(level):
        cap1, cap2, near1, near2 = caps = levels[level]
        counts1 = [cap1] * half + [near1] * half
        counts2 = [cap2] * half + [near2] * half
        batches = [(count + slots * (BATCH - 1)) // BATCH for count in counts2]

        def run(*values):
            return pl.pallas_call(
                functools.partial(packed_kernel, groups, lanes, pair, full, caps, cuts, base),
                out_shape=jax.ShapeDtypeStruct((held * share, UNIT, width * lanes), bf16),
                in_specs=[smem, vmem] + [anywhere] * 5 + [vmem, vmem],
                out_specs=vmem,
                scratch_shapes=[
                    *(pltpu.VMEM((pair, count, UNIT, wide), bf16) for count in counts1),
                    *(pltpu.VMEM((pair, count, UNIT, wide), bf16) for count in counts1),
                    *(pltpu.VMEM((count * BATCH, UNIT, wide), bf16) for count in batches),
                    *(pltpu.VMEM((sum(counts2), UNIT, cut), bf16) for cut in cuts),
                    *(pltpu.VMEM((sum(counts2), UNIT, cut), bf16) for cut in cuts),
                    *(pltpu.VMEM((pair, lanes, held * share, UNIT, cut), bf16) for cut in cuts),
                    pltpu.VMEM((slots, prefix, HEAD), bf16),
                    pltpu.VMEM((slots, prefix, HEAD), bf16),
                    dma((planes, pair)), dma((planes, pair)), dma((4,)), dma((len(base),)),
                    dma((PIECES, planes)), dma((PIECES, planes)),
                    dma((PIECES, pair, lanes)), dma((PIECES, pair, lanes)),
                ],
                compiler_params=pltpu.CompilerParams(
                    collective_id=2 + level, has_side_effects=True
                ),
                name=f"packed_prefix_attention_{level}",
            )(*values)

        return run

    out = lax.switch(
        chosen.reshape(()), [branch(level) for level in range(len(levels))], *operands
    )
    return out.reshape(held, share * UNIT, width * lanes)


def fits(groups, lanes, queries, prefix_keys):
    held, rows, width = queries.shape
    pair = prefix_keys.shape[2] // HEAD
    if pair != 2 or groups // pair not in (2, 4) or groups % (2 * pair):
        return False
    if rows % (UNIT * lanes) or rows >= LANES:
        return False
    planes = groups // pair
    spots = planes * planes * pair * prefix_keys.shape[0]
    full_plane = CAPC * pair * pair * rows // UNIT
    room = full_plane + pair * prefix_keys.shape[0] * (BATCH - 1)
    return groups * held <= LANES and spots <= LANES and room <= LANES


def local(groups, lanes, queries, prefix_keys, *rest):
    form = packed if fits(groups, lanes, queries, prefix_keys) else padded
    return form(groups, lanes, queries, prefix_keys, *rest)


def solution(mesh):
    placed = (
        P("group", None, "tensor"),
        P("group", None, "tensor"),
        P("group", None, "tensor"),
        P(),
        P("group"),
        P("group"),
    )
    return jax.shard_map(
        functools.partial(local, mesh.shape["group"], mesh.shape["tensor"]),
        mesh=mesh, in_specs=placed, out_specs=P("group", "tensor", None), check_vma=False,
    )
```

```python
import functools
import math

import numpy as np

import jax
import jax.numpy as jnp
from jax import lax
from jax.experimental import pallas as pl
from jax.experimental.pallas import tpu as pltpu
from jax.sharding import PartitionSpec as P

HEAD = 128
CAPC = 2
ROTARY_BASE = 1000000.0
TILE = 16
UNIT = 8
BATCH = 4
LANES = 128
MESH = pl.DeviceIdType.MESH
PIECES = 3
LEVELS = (
    (0.65625, 0.4375, 0.6875, 0.5625, 0.4286, 0.4286),
    (0.65625, 0.5, 0.75, 0.59375, 0.4571, 0.4571),
    (0.65625, 0.5625, 0.75, 0.625, 0.4857, 0.4857),
    (0.75, 0.5, 0.8125, 0.625, 0.4857, 0.4857),
    (0.75, 0.5625, 0.875, 0.6875, 0.5143, 0.5143),
    (0.84375, 0.65625, 0.9375, 0.75, 0.5429, 0.5429),
    (1, 1, 1, 1, 1.0000, 1.0000),
)


def rotary_tables(first_position, rows):
    half = HEAD // 2
    frequencies = np.float32(ROTARY_BASE) ** (
        -(np.arange(half, dtype=np.float32) * np.float32(2.0) / np.float32(HEAD))
    )
    positions = (first_position + np.arange(rows)).astype(np.float32)
    angles = (positions[:, None] * frequencies.astype(np.float32)[None, :]).astype(np.float64)
    cos, sin = np.cos(angles), np.sin(angles)
    return (
        np.concatenate([cos, cos], axis=1).astype(np.float32),
        np.concatenate([-sin, sin], axis=1).astype(np.float32),
    )


def padded_kernel(
    groups, lanes, moved,
    source_ref, tag_ref, dest_ref, length_ref,
    q_ref, k_ref, v_ref, cos_ref, sin_ref,
    out_ref,
    q_out, q_in, sel_out, sel_in, res, stage,
    q_send, q_recv, s_send, s_recv, r_send, r_recv,
    *near,
):
    me, lane = lax.axis_index("group"), lax.axis_index("tensor")
    held, rows, width = q_ref.shape
    cached, prefix, kv_width = k_ref.shape
    share = rows // lanes
    kv_local = kv_width // HEAD
    per_kv = width // HEAD // kv_local
    half = groups // 2
    factor = math.log2(math.e) / math.sqrt(HEAD)
    wide_near = moved * per_kv * HEAD
    if moved:
        (n_out, n_in, ns_out, ns_in, n_res, k_far, v_far,
         n_send, n_recv, ns_send, ns_recv, nr_send, nr_recv, kv_send, kv_recv) = near
    spot = lax.rem(me, half)
    base = me - spot
    mirror = lax.rem(me + half, groups)

    barrier = pltpu.get_barrier_semaphore()

    def greet(step, carry):
        for turn in range(lanes):
            def send():
                pl.semaphore_signal(
                    barrier, inc=1,
                    device_id=(lax.rem(me + step, groups), lax.rem(lane + turn, lanes)),
                    device_id_type=MESH,
                )
            if turn:
                send()
            else:
                pl.when(step > 0)(send)
        return carry

    lax.fori_loop(0, groups, greet, 0)

    def offset_of(step):
        swing = (step + 1) // 2
        return lax.rem(half + (1 - 2 * lax.rem(step, 2)) * swing + groups, groups)

    def route(owner):
        places = [owner * CAPC + slot for slot in range(CAPC)]
        return [(source_ref[place], tag_ref[place]) for place in places]

    def fill(items, q_to, sel_to, block, first, last):
        for slot, (item, tag) in enumerate(items):
            for j in range(cached):
                weight = jnp.where(tag == j, 1.0, 0.0)
                sel_to[block, slot * cached + j] = jnp.full(
                    (TILE, HEAD), weight, jnp.float32
                ).astype(jnp.bfloat16)
            for head in range(first, last):
                x = q_ref[item, :, head * HEAD:(head + 1) * HEAD].astype(jnp.float32)
                turned = x * cos_ref[...] + pltpu.roll(x, HEAD // 2, 1) * sin_ref[...]
                span = slice((head - first) * HEAD, (head - first + 1) * HEAD)
                q_to[block, slot, :, span] = turned.astype(jnp.bfloat16)

    near_heads, all_heads = moved * per_kv, width // HEAD

    def pair(src, dst, send_sem, recv_sem, device):
        return pltpu.make_async_remote_copy(
            src_ref=src, dst_ref=dst, send_sem=send_sem, recv_sem=recv_sem,
            device_id=device, device_id_type=MESH,
        )

    def q_copies(here, there, device):
        return (
            pair(sel_out.at[here], sel_in.at[there], s_send.at[here], s_recv.at[there],
                 (device, lane)),
            pair(q_out.at[here], q_in.at[there], q_send.at[here], q_recv.at[there],
                 (device, lane)),
        )

    def n_copies(here, there, device):
        return (
            pair(ns_out.at[here], ns_in.at[there], ns_send.at[here], ns_recv.at[there],
                 (device, lane)),
            pair(n_out.at[here], n_in.at[there], n_send.at[here], n_recv.at[there],
                 (device, lane)),
        )

    def place(owner, from_lane, skip, wide):
        start = pl.multiple_of(from_lane * width + skip, HEAD)
        return stage.at[pl.ds(owner * CAPC, CAPC), :, pl.ds(start, wide)]

    def r_copy(block, piece, owner, from_lane, device):
        return pair(
            res.at[block, :, piece], place(owner, from_lane, wide_near, width - wide_near),
            r_send.at[block, piece], r_recv.at[owner, from_lane], (device, piece),
        )

    def nr_copy(block, piece, owner, from_lane, device):
        return pair(
            n_res.at[block, :, piece], place(owner, from_lane, 0, wide_near),
            nr_send.at[block, piece], nr_recv.at[owner, from_lane], (device, piece),
        )

    def kv_copies():
        span = pl.ds(0, moved * HEAD)
        return (
            pair(k_ref.at[:, :, span], k_far, kv_send.at[0], kv_recv.at[0], (mirror, lane)),
            pair(v_ref.at[:, :, span], v_far, kv_send.at[1], kv_recv.at[1], (mirror, lane)),
        )

    items = route(mirror)
    fill(items, q_out, sel_out, mirror, near_heads, all_heads)
    pl.semaphore_wait(barrier, groups * lanes - 1)
    for copy in q_copies(mirror, me, mirror):
        copy.start()
    if moved:
        fill(items, n_in, ns_in, spot + half, 0, near_heads)

    def dispatch(step, carry):
        owner = lax.rem(me + offset_of(step), groups)
        items = route(owner)
        fill(items, q_out, sel_out, owner, near_heads, all_heads)
        for copy in q_copies(owner, me, owner):
            copy.start()
        if moved:
            fill(items, n_out, ns_out, owner, 0, near_heads)
            seat = lax.rem(owner, half)
            kind = lax.rem(lax.div(owner, half) + lax.div(me, half), 2)
            for copy in n_copies(owner, spot + half * kind, base + seat):
                copy.start()
        return carry

    lax.fori_loop(1, groups - 1, dispatch, 0)
    if moved:
        for copy in kv_copies():
            copy.start()
    items = route(me)
    fill(items, q_in, sel_in, me, near_heads, all_heads)
    if moved:
        fill(items, n_in, ns_in, spot, 0, near_heads)

    def attend(q_from, sel_from, to, block, keys, values, first, count):
        for slot in range(CAPC):
            weights = [sel_from[block, slot * cached + j][None] for j in range(cached)]

            def chosen(ref, span):
                total = None
                for j in range(cached):
                    part = ref[j, :, span].reshape(prefix // TILE, TILE, HEAD) * weights[j]
                    total = part if total is None else total + part
                return total.reshape(prefix, HEAD)

            for kv in range(count):
                span = slice((first + kv) * HEAD, (first + kv + 1) * HEAD)
                spans = [
                    slice((kv * per_kv + g) * HEAD, (kv * per_kv + g + 1) * HEAD)
                    for g in range(per_kv)
                ]
                query = jnp.concatenate([q_from[block, slot, :, s] for s in spans], axis=0)
                scores = lax.dot_general(
                    query, chosen(keys, span), (((1,), (1,)), ((), ())),
                    preferred_element_type=jnp.float32,
                )
                peak = jnp.max(scores, axis=-1, keepdims=True)
                weight = jnp.exp2((scores - peak) * factor)
                total = jnp.sum(weight, axis=-1, keepdims=True)
                mixed = jnp.dot(
                    weight.astype(jnp.bfloat16), chosen(values, span),
                    preferred_element_type=jnp.float32,
                )
                mixed = (mixed / total).astype(jnp.bfloat16)
                for g in range(per_kv):
                    to[block, slot, :, :, spans[g]] = mixed[g * rows:(g + 1) * rows].reshape(
                        lanes, share, HEAD
                    )

    def give_back(step, copy, source, block, owner, done, skip, wide):
        for turn in range(1, lanes):
            copy(block, lax.rem(lane + turn, lanes), owner, lane, source).start()

        @pl.when(step > 0)
        def _():
            copy(block, lane, owner, lane, source).start()

        @pl.when(step == 0)
        def _():
            start = pl.multiple_of(lane * width + skip, HEAD)
            stage[pl.ds(owner * CAPC, CAPC), :, pl.ds(start, wide)] = done[block, :, lane]

    def far_work(step, carry):
        source = lax.rem(me + groups - offset_of(lax.rem(step + groups - 1, groups)), groups)

        @pl.when(step > 0)
        def _():
            for copy in q_copies(source, source, source):
                copy.wait_recv()

        attend(q_in, sel_in, res, source, k_ref, v_ref, moved, kv_local - moved)
        give_back(step, r_copy, source, source, me, res, wide_near, width - wide_near)
        return carry

    def near_work(kind, keys, values, owner):
        def body(step, carry):
            seat = lax.rem(spot + step, half)
            block = seat + half * kind

            @pl.when(step > 0)
            def _():
                for copy in n_copies(block, block, base + seat):
                    copy.wait_recv()

            attend(n_in, ns_in, n_res, block, keys, values, 0, moved)
            give_back(step, nr_copy, base + seat, block, owner, n_res, 0, wide_near)
            return carry

        lax.fori_loop(0, half, body, 0)

    if moved:
        near_work(0, k_ref, v_ref, me)
    lax.fori_loop(0, groups, far_work, 0)
    if moved:
        for copy in kv_copies():
            copy.wait_recv()
        near_work(1, k_far, v_far, mirror)

    def returned(step, copy, block, owner, device):
        @pl.when(step > 0)
        def _():
            copy(block, lane, owner, lane, device).wait_send()
            copy(block, lane, owner, lane, device).wait_recv()

        for turn in range(1, lanes):
            piece = lax.rem(lane + turn, lanes)
            copy(block, piece, owner, piece, device).wait_send()
            copy(block, piece, owner, piece, device).wait_recv()

    def far_settle(step, carry):
        other = lax.rem(me + step, groups)

        @pl.when(step > 0)
        def _():
            for copy in q_copies(other, me, other):
                copy.wait_send()

        returned(step, r_copy, other, other, other)
        return carry

    lax.fori_loop(0, groups, far_settle, 0)
    if moved:
        for copy in kv_copies():
            copy.wait_send()

        def near_settle(step, carry):
            seat = lax.rem(spot + step, half)
            for kind in range(2):
                owner = lax.rem(base + half * kind, groups) + seat

                @pl.when(step > 0)
                def _():
                    for copy in n_copies(owner, owner, base + seat):
                        copy.wait_send()

                returned(step, nr_copy, seat + half * kind, owner, base + seat)
            return carry

        lax.fori_loop(0, half, near_settle, 0)

    def deliver(item, carry):
        found = stage[dest_ref[item]].astype(jnp.float32)
        position = lane * share + lax.broadcasted_iota(jnp.int32, found.shape, 0)
        out_ref[item] = jnp.where(position < length_ref[item], found, 0.0).astype(jnp.bfloat16)
        return carry

    lax.fori_loop(0, held, deliver, 0)


def padded(groups, lanes, queries, prefix_keys, prefix_values, slot_of_prompt, prompt_of, lengths):
    held, rows, width = queries.shape
    cached, prefix, kv_width = prefix_keys.shape
    share = rows // lanes
    kv_local = kv_width // HEAD
    moved = kv_local // 2 if groups % 2 == 0 and groups >= 4 else 0
    wide_near = moved * (width // kv_local)
    wide = width - wide_near
    cos, sin = rotary_tables(prefix, rows)
    cache_rows = slot_of_prompt[prompt_of]
    owner = cache_rows // cached
    serial = jnp.arange(held)
    earlier = (owner[None, :] == owner[:, None]) & (serial[None, :] < serial[:, None])
    destination = owner * CAPC + jnp.sum(earlier.astype(jnp.int32), axis=1)
    matches = destination[None, :] == jnp.arange(groups * CAPC)[:, None]
    source = jnp.sum(jnp.where(matches, serial[None, :], 0), axis=1)
    tags = jnp.sum(jnp.where(matches, (cache_rows % cached)[None, :], 0), axis=1)
    smem = pl.BlockSpec(memory_space=pltpu.SMEM)
    vmem = pl.BlockSpec(memory_space=pltpu.VMEM)
    dma = pltpu.SemaphoreType.DMA
    bf16 = jnp.bfloat16

    def exchange(features):
        return [
            pltpu.VMEM((groups, CAPC, rows, features), bf16),
            pltpu.VMEM((groups, CAPC, rows, features), bf16),
            pltpu.VMEM((groups, CAPC * cached, TILE, HEAD), bf16),
            pltpu.VMEM((groups, CAPC * cached, TILE, HEAD), bf16),
            pltpu.VMEM((groups, CAPC, lanes, share, features), bf16),
        ]

    semaphores = [
        dma((groups,)), dma((groups,)),
        dma((groups,)), dma((groups,)),
        dma((groups, lanes)), dma((groups, lanes)),
    ]
    scratch = [
        *exchange(wide),
        pltpu.VMEM((groups * CAPC, share, width * lanes), bf16),
        *semaphores,
    ]
    if moved:
        scratch += [
            *exchange(wide_near),
            pltpu.VMEM((cached, prefix, moved * HEAD), bf16),
            pltpu.VMEM((cached, prefix, moved * HEAD), bf16),
            *semaphores,
            dma((2,)), dma((2,)),
        ]
    return pl.pallas_call(
        functools.partial(padded_kernel, groups, lanes, moved),
        out_shape=jax.ShapeDtypeStruct((held, share, width * lanes), bf16),
        in_specs=[smem] * 4 + [vmem] * 5,
        out_specs=vmem,
        scratch_shapes=scratch,
        compiler_params=pltpu.CompilerParams(collective_id=0, has_side_effects=True),
        name="routed_prefix_attention",
    )(
        source.astype(jnp.int32), tags.astype(jnp.int32), destination.astype(jnp.int32), lengths,
        queries, prefix_keys, prefix_values, jnp.asarray(cos), jnp.asarray(sin),
    )


def xor_order(step, plane, planes):
    half = planes // 2
    near = lax.div(step, half)
    side = lax.rem(lax.div(plane, half) + 1 - near, 2)
    return side * half + lax.rem(lax.rem(plane, half) + step + near, half)


def step_of(plane, z, planes):
    half = planes // 2
    shift = lax.rem(plane + planes - z, half)
    far = shift
    near = half + lax.rem(shift + half - 1, half)
    return jnp.where(plane // half != z // half, far, near)


def plan_kernel(
    groups, pair, levels, full, base,
    slot_ref, prompt_ref, length_ref, q_ref, k_ref, v_ref, cos_ref, sin_ref,
    tables_ref, level_ref, k_far, v_far, q_base,
    mine, gathered, q_out, send, recv, q_send, q_recv, kv_send, kv_recv,
):
    shared = len(base)
    me, lane = lax.axis_index("group"), lax.axis_index("tensor")
    held = prompt_ref.shape[0]
    slots = slot_ref.shape[0]
    planes = groups // pair
    per_plane = slots // planes
    total = groups * held
    full_pair, full_plane = full
    turns = full_pair // (CAPC * pair)
    half = planes // 2
    z, x = lax.div(me, pair), lax.rem(me, pair)
    partner = z * pair + 1 - x
    there = [xor_order(step, z, planes) for step in range(shared)]
    barrier = pltpu.get_barrier_semaphore()

    def greet(step, carry):
        pl.semaphore_signal(
            barrier, inc=1, device_id=(lax.rem(me + step, groups), lane), device_id_type=MESH
        )
        return carry

    lax.fori_loop(1, groups, greet, 0)

    def remote(src, dst, send_sem, recv_sem, group):
        return pltpu.make_async_remote_copy(
            src_ref=src, dst_ref=dst, send_sem=send_sem, recv_sem=recv_sem,
            device_id=(group, lane), device_id_type=MESH,
        )

    span = pl.ds(pl.multiple_of((1 - x) * HEAD, HEAD), HEAD)
    kv_copies = [
        remote(ref.at[:, :, span], far_ref, kv_send.at[i], kv_recv.at[i], partner)
        for i, (ref, far_ref) in enumerate(((k_ref, k_far), (v_ref, v_far)))
    ]

    def q_copy(step, j, source, device):
        return remote(
            q_out.at[step, j, pl.ds(0, base[step])], q_base.at[step, source, pl.ds(0, base[step])],
            q_send.at[step, j], q_recv.at[step, source], device,
        )

    own_slots = [slot_ref[prompt_ref[i]] for i in range(held)]
    own_planes = [lax.div(slot, per_plane) for slot in own_slots]
    own_counts = [lax.div(length_ref[i] + UNIT - 1, UNIT) for i in range(held)]
    own_starts = []
    for i in range(held):
        start = jnp.int32(0)
        for other in range(i):
            start = start + jnp.where(own_planes[other] == own_planes[i], own_counts[other], 0)
        own_starts.append(start)

    def fill(step):
        starts = [
            jnp.where(own_planes[i] == there[step], own_starts[i], LANES) for i in range(held)
        ]

        def one(k, carry):
            index = jnp.int32(0)
            for i in range(held):
                offset = k - starts[i]
                hit = (offset >= 0) & (offset < own_counts[i])
                index = index + jnp.where(hit, i * turns + offset, 0)
            rope(index, q_ref, cos_ref, sin_ref, q_out.at[step], k, pair)
            return carry

        lax.fori_loop(0, base[step], one, 0)

    lanes1 = lax.broadcasted_iota(jnp.int32, (1, LANES), 1)
    row = jnp.zeros((1, LANES), jnp.int32)
    for i in range(held):
        value = own_slots[i] * LANES + length_ref[i]
        row = jnp.where(lanes1 == me * held + i, value, row)
    mine[...] = row
    gathered[me] = row
    for step in range(half):
        fill(step)
    pl.semaphore_wait(barrier, groups - 1)

    def copy(there, device):
        return pltpu.make_async_remote_copy(
            src_ref=mine, dst_ref=gathered.at[there], send_sem=send.at[device],
            recv_sem=recv.at[there], device_id=(device, lane), device_id_type=MESH,
        )

    def push(step, carry):
        copy(me, lax.rem(me + step, groups)).start()
        return carry

    lax.fori_loop(1, groups, push, 0)

    def dispatch(step):
        for j in range(pair):
            q_copy(step, j, x, there[step] * pair + j).start()

    for step in range(half):
        dispatch(step)
    for kv_copy in kv_copies:
        kv_copy.start()
    for step in range(half, shared):
        fill(step)
        dispatch(step)

    def settle(step, carry):
        other = lax.rem(me + step, groups)
        copy(other, other).wait_recv()
        copy(me, other).wait_send()
        return carry

    lax.fori_loop(1, groups, settle, 0)
    code = gathered[0]
    for g in range(1, groups):
        code = code + gathered[g]

    square = (LANES, LANES)
    down = lax.broadcasted_iota(jnp.int32, square, 0)
    across = lax.broadcasted_iota(jnp.int32, square, 1)
    eye = down == across

    def to_column(values):
        return jnp.sum(jnp.where(eye, jnp.broadcast_to(values, square), 0), axis=1, keepdims=True)

    def to_row(values):
        return jnp.sum(jnp.where(eye, jnp.broadcast_to(values, square), 0), axis=0, keepdims=True)

    def facts(values, index):
        live = index < total
        length = values % LANES
        slot = values // LANES
        count = jnp.where(live, (length + UNIT - 1) // UNIT, 0)
        return count, slot, slot // per_plane, index // held, index // (held * pair)

    col = to_column(code)
    down1 = lax.broadcasted_iota(jnp.int32, (LANES, 1), 0)
    count_r, slot_r, to_r, from_r, plane_r = facts(code, lanes1)
    count_c, slot_c, to_c, from_c, plane_c = facts(col, down1)
    weight = jnp.broadcast_to(count_c, square)
    earlier = (down < across) & (to_c == to_r)

    def rank(mask):
        return jnp.sum(jnp.where(mask, weight, 0), axis=0, keepdims=True)

    base1 = rank(earlier & (from_c == from_r))
    base2 = rank(earlier & (plane_c == plane_r))
    side_r = jnp.where(plane_r // half == to_r // half, 1, 0)
    side_c = jnp.where(plane_c // half == to_c // half, 1, 0)
    within = rank(earlier & (side_c == side_r) & (slot_c == slot_r))
    key_r = side_r * slots + slot_r
    number = jnp.sum(
        jnp.where(down1 == key_r, jnp.broadcast_to(count_r, square), 0), axis=1, keepdims=True
    )
    need = (number + BATCH - 1) // BATCH
    need_r = to_row(need)
    first = jnp.sum(
        jnp.where(
            (down // per_plane == across // per_plane) & (across < down),
            jnp.broadcast_to(need_r, square), 0,
        ),
        axis=1, keepdims=True,
    )
    first_of = jnp.sum(
        jnp.where(down1 == key_r, jnp.broadcast_to(first, square), 0), axis=0, keepdims=True
    )
    place = first_of * BATCH + within
    base1_c, base2_c, place_c = to_column(base1), to_column(base2), to_column(place)

    alive = lanes1 < total
    far = alive & (to_r // half != plane_r // half)
    near = alive & (to_r // half == plane_r // half)
    needs = [
        jnp.max(jnp.where(mask, begin + count_r, 0))
        for mask in (far, near) for begin in (base1, base2)
    ] + [jnp.max(jnp.where(down1 // slots == side, first + need, 0)) for side in range(2)]
    level = jnp.int32(len(levels) - 1)
    for index, caps in reversed(list(enumerate(levels[:-1]))):
        over = needs[0] > caps[0]
        for value, cap in zip(needs[1:], caps[1:]):
            over = over | (value > cap)
        level = jnp.where(over, level, index)
    level_ref[0] = level
    tables_ref[pl.ds(1, 1), :] = code
    tables_ref[pl.ds(2, 1), :] = step_of(to_r, z, planes) * full_plane + base2

    def pick(mask, start_c, value_c, index):
        hit = mask & (index >= start_c) & (index < start_c + count_c)
        return jnp.sum(jnp.where(hit, value_c + index, 0), axis=0, keepdims=True)

    for plane in range(planes):
        tables_ref[pl.ds(3 + plane, 1), :] = pick(
            (from_c == me) & (to_c == plane), base1_c,
            lax.rem(down1, held) * turns - base1_c, lanes1,
        )
        tables_ref[pl.ds(3 + planes + plane, 1), :] = pick(
            (plane_c == plane) & (to_c == z), base2_c, place_c - base2_c, lanes1
        )
    seat_c = lax.rem(step_of(plane_c, z, planes), half) * pair + lax.rem(from_c, pair)
    for side in range(2):
        for page in range(2):
            tables_ref[pl.ds(3 + 2 * planes + 2 * side + page, 1), :] = pick(
                (side_c == side) & (to_c == z), place_c,
                seat_c * full_pair + base1_c - place_c, lanes1 + page * LANES,
            )
        starts = (
            (down1 // slots == side) & (lax.rem(down1, slots) // per_plane == z)
            & (lanes1 >= first) & (lanes1 < first + need)
        )
        tables_ref[pl.ds(7 + 2 * planes + side, 1), :] = jnp.sum(
            jnp.where(starts, lax.rem(down1, per_plane), 0), axis=0, keepdims=True
        )
    for step in range(shared):
        for j in range(pair):
            q_copy(step, j, j, me).wait_recv()
            q_copy(step, j, x, there[step] * pair + j).wait_send()
    for kv_copy in kv_copies:
        kv_copy.wait_recv()
        kv_copy.wait_send()


def rope(index, q_ref, cos_ref, sin_ref, to, k, pair):
    turn = lax.rem(index, cos_ref.shape[0])
    cos, sin = cos_ref[turn], sin_ref[turn]
    block = q_ref[index].astype(jnp.float32)
    per_kv = block.shape[-1] // HEAD // pair
    for j in range(pair):
        parts = []
        for g in range(per_kv):
            head = j * per_kv + g
            part = block[:, head * HEAD:(head + 1) * HEAD]
            turned = part * cos + pltpu.roll(part, HEAD // 2, 1) * sin
            parts.append(turned.astype(jnp.bfloat16))
        to[j, k] = jnp.concatenate(parts, axis=1)


def packed_kernel(
    groups, lanes, pair, full, caps, cuts, base,
    tables,
    q_ref, k_ref, v_ref, k_far, v_far, q_base, cos_ref, sin_ref,
    out_ref,
    *scratch,
):
    me, lane = lax.axis_index("group"), lax.axis_index("tensor")
    planes = groups // pair
    half = planes // 2
    pieces = len(cuts)
    scratch = list(scratch)

    def take(count):
        taken = scratch[:count]
        del scratch[:count]
        return taken

    q_out, q_sides, results = take(planes), take(2), take(2)
    q_in = [q_sides[step // half].at[step % half] for step in range(planes)]
    r_out, r_in, stage = take(pieces), take(pieces), take(pieces)
    k_all, v_all = take(2)
    q_send, q_recv, kv_here, q_here, r_send, r_recv, f_send, f_recv = scratch

    z, x = lax.div(me, pair), lax.rem(me, pair)
    cached, prefix, _ = k_ref.shape
    units, _, width = q_ref.shape
    wide = width // pair
    per_kv = wide // HEAD
    turns = cos_ref.shape[0]
    held = units // turns
    share = turns // lanes
    full_pair, full_plane = full
    cap1, cap2, near1, near2 = caps[:4]
    factor = math.log2(math.e) / math.sqrt(HEAD)
    send_row, ret_row, comp_row, slot_row = 3, 3 + planes, 3 + 2 * planes, 7 + 2 * planes
    counts1 = [cap1 if step < half else near1 for step in range(planes)]
    counts2 = [cap2 if step < half else near2 for step in range(planes)]
    offsets = [sum(counts2[:step]) for step in range(planes)]
    last = planes - 1
    there = [xor_order(step, z, planes) for step in range(planes)]

    barrier = pltpu.get_barrier_semaphore()

    def greet(step, carry):
        pl.semaphore_signal(
            barrier, inc=1, device_id=(lax.rem(me + step, groups), lane), device_id_type=MESH
        )
        return carry

    lax.fori_loop(1, groups, greet, 0)
    for turn in range(1, lanes):
        for j in range(pair):
            pl.semaphore_signal(
                barrier, inc=1,
                device_id=(z * pair + j, lax.rem(lane + turn, lanes)), device_id_type=MESH,
            )

    def span_of(j):
        return pl.ds(pl.multiple_of(j * HEAD, HEAD), HEAD)

    here = [
        pltpu.make_async_copy(
            ref.at[:, :, span_of(x)], full_ref.at[pl.ds(x * cached, cached)], kv_here.at[i]
        )
        for i, (ref, full_ref) in enumerate(((k_ref, k_all), (v_ref, v_all)))
    ] + [
        pltpu.make_async_copy(
            far_ref, full_ref.at[pl.ds((1 - x) * cached, cached)], kv_here.at[2 + i]
        )
        for i, (far_ref, full_ref) in enumerate(((k_far, k_all), (v_far, v_all)))
    ] + [
        pltpu.make_async_copy(
            q_base.at[step, :, pl.ds(0, base[step])], q_in[step].at[:, pl.ds(0, base[step])],
            q_here.at[step],
        )
        for step in range(len(base))
    ]
    for copy in here:
        copy.start()

    def remote(src, dst, send_sem, recv_sem, group, to_lane):
        return pltpu.make_async_remote_copy(
            src_ref=src, dst_ref=dst, send_sem=send_sem, recv_sem=recv_sem,
            device_id=(group, to_lane), device_id_type=MESH,
        )

    rest = [
        slice(base[step] if step < len(base) else 0, counts1[step]) for step in range(planes)
    ]

    def q_copy(step, j, source, device):
        span = pl.ds(rest[step].start, rest[step].stop - rest[step].start)
        return remote(
            q_out[step].at[j, span], q_in[step].at[source, span], q_send.at[step, j],
            q_recv.at[step, source], device, lane,
        )

    def fill(step):
        def one(k, carry):
            index = tables[send_row + there[step], k]
            rope(index, q_ref, cos_ref, sin_ref, q_out[step], k, pair)
            return carry

        lax.fori_loop(rest[step].start, rest[step].stop, one, 0)

    moving = [step for step in range(planes) if rest[step].stop > rest[step].start]

    def dispatch(step):
        if step not in moving:
            return
        for j in range(pair):
            if step < last:
                q_copy(step, j, x, there[step] * pair + j).start()
            else:
                @pl.when(j != x)
                def _():
                    q_copy(step, j, x, there[step] * pair + j).start()

    for step in moving:
        fill(step)
    q_in[last][x] = q_out[last][x]

    def greeted():
        pl.semaphore_wait(barrier, groups - 1 + pair * (lanes - 1))
        for step in moving:
            dispatch(step)

    if 0 in moving:
        greeted()
    for copy in here:
        copy.wait()

    def r_copy(piece, step):
        region = pl.ds(offsets[step], counts2[step])
        return remote(
            r_out[piece].at[region], r_in[piece].at[region],
            r_send.at[piece, step], r_recv.at[piece, step], there[step] * pair + x, lane,
        )

    for side in range(2):
        steps = range(side * half, side * half + half)
        for step in steps:
            for j in range(pair) if step in moving else []:
                if step < last:
                    q_copy(step, j, j, me).wait_recv()
                else:
                    @pl.when(j != x)
                    def _():
                        q_copy(step, j, j, me).wait_recv()

        def batch(b, carry):
            slot = tables[slot_row + side, b]
            blocks = []
            for i in range(BATCH):
                entry = b * BATCH + i
                index = tables[
                    comp_row + 2 * side + lax.div(entry, LANES), lax.rem(entry, LANES)
                ]
                seat = lax.div(index, full_pair)
                blocks.append(
                    q_sides[side][
                        lax.div(seat, pair), lax.rem(seat, pair), lax.rem(index, full_pair)
                    ].astype(jnp.float32)
                )
            query = jnp.concatenate(
                [block[:, g * HEAD:(g + 1) * HEAD] for g in range(per_kv) for block in blocks],
                axis=0,
            ).astype(jnp.bfloat16)
            scores = lax.dot_general(
                query, k_all[slot], (((1,), (1,)), ((), ())), preferred_element_type=jnp.float32
            )
            peak = jnp.max(scores, axis=-1, keepdims=True)
            weight = jnp.exp2((scores - peak) * factor)
            total = jnp.sum(weight, axis=-1, keepdims=True)
            mixed = jnp.dot(
                weight.astype(jnp.bfloat16), v_all[slot], preferred_element_type=jnp.float32
            ) / total
            for i in range(BATCH):
                results[side][b * BATCH + i] = jnp.concatenate(
                    [
                        mixed[(g * BATCH + i) * UNIT:(g * BATCH + i + 1) * UNIT]
                        for g in range(per_kv)
                    ],
                    axis=1,
                ).astype(jnp.bfloat16)
            return carry

        lax.fori_loop(0, results[side].shape[0] // BATCH, batch, 0, unroll=2)
        if side == 0 and 0 not in moving:
            greeted()
        for step in steps:
            target = r_out if step < last else r_in

            def pack(k, carry):
                found = results[side][tables[ret_row + there[step], k]]
                start = 0
                for piece in range(pieces):
                    target[piece][offsets[step] + k] = found[:, start:start + cuts[piece]]
                    start += cuts[piece]
                return carry

            lax.fori_loop(0, counts2[step], pack, 0, unroll=2)
            if step < last:
                r_copy(0, step).start()
            if step == half - 1:
                for piece in range(1, pieces):
                    for ready in range(half):
                        r_copy(piece, ready).start()
            if step == last - 1:
                for piece in range(1, pieces):
                    for ready in range(half, last):
                        r_copy(piece, ready).start()

    def lineup(step):
        return lax.rem(x + step + 1, pair), lax.rem(lane + lax.div(step + 1, pair), lanes)

    def final(piece, at_x, at_lane, from_x, from_lane, to_x, to_lane):
        skip = sum(cuts[:piece])
        start = pl.multiple_of((from_lane * pair + from_x) * wide + skip, HEAD)
        return remote(
            stage[piece].at[at_x, at_lane], out_ref.at[:, :, pl.ds(start, cuts[piece])],
            f_send.at[piece, at_x, at_lane], f_recv.at[piece, from_x, from_lane],
            z * pair + to_x, to_lane,
        )

    for piece in range(pieces):
        for step in range(last):
            r_copy(piece, step).wait_recv()

        def spread(step, carry):
            to_x, to_lane = lineup(step)

            def one(i, inner):
                item = (z * pair + to_x) * held + i
                entry = tables[2, item]
                length = lax.rem(tables[1, item], LANES)
                source, rank = lax.div(entry, full_plane), lax.rem(entry, full_plane)
                cap = jnp.where(source < half, cap2, near2)
                offset = jnp.where(
                    source < half, source * cap2, half * cap2 + (source - half) * near2
                )
                for s in range(share):
                    unit = to_lane * share + s
                    found = r_in[piece][offset + jnp.minimum(rank + unit, cap - 1)].astype(
                        jnp.float32
                    )
                    row = unit * UNIT + lax.broadcasted_iota(jnp.int32, found.shape, 0)
                    stage[piece][to_x, to_lane, i * share + s] = jnp.where(
                        row < length, found, 0.0
                    ).astype(jnp.bfloat16)
                return inner

            lax.fori_loop(0, held, one, 0, unroll=2)

            @pl.when(step < pair * lanes - 1)
            def _():
                final(piece, to_x, to_lane, x, lane, to_x, to_lane).start()
            return carry

        lax.fori_loop(0, pair * lanes, spread, 0)
        start = pl.multiple_of((lane * pair + x) * wide + sum(cuts[:piece]), HEAD)
        out_ref[:, :, pl.ds(start, cuts[piece])] = stage[piece][x, lane]

    def drain(step, carry):
        to_x, to_lane = lineup(step)
        for piece in range(pieces):
            final(piece, to_x, to_lane, to_x, to_lane, to_x, to_lane).wait_recv()
            final(piece, to_x, to_lane, x, lane, to_x, to_lane).wait_send()
        return carry

    lax.fori_loop(0, pair * lanes - 1, drain, 0)
    for step in range(planes):
        for j in range(pair) if step in moving else []:
            if step < last:
                q_copy(step, j, x, there[step] * pair + j).wait_send()
            else:
                @pl.when(j != x)
                def _():
                    q_copy(step, j, x, there[step] * pair + j).wait_send()
        if step < last:
            for piece in range(pieces):
                r_copy(piece, step).wait_send()


def packed(groups, lanes, queries, prefix_keys, prefix_values, slot_of_prompt, prompt_of, lengths):
    held, rows, width = queries.shape
    cached, prefix, kv_width = prefix_keys.shape
    pair = kv_width // HEAD
    planes = groups // pair
    half = planes // 2
    turns = rows // UNIT
    full_pair = CAPC * pair * turns
    full_plane = full_pair * pair
    slots = cached * pair
    full_side = (full_plane * half + slots * (BATCH - 1)) // BATCH
    share = turns // lanes
    wide = width // pair
    per_kv = wide // HEAD
    cuts = [HEAD * (per_kv // PIECES + (i < per_kv % PIECES)) for i in range(PIECES)]
    levels = [
        tuple(
            round(whole * part)
            for whole, part in zip((full_pair, full_plane) * 2 + (full_side, full_side), level)
        )
        for level in LEVELS
    ]
    smem = pl.BlockSpec(memory_space=pltpu.SMEM)
    vmem = pl.BlockSpec(memory_space=pltpu.VMEM)
    anywhere = pl.BlockSpec(memory_space=pl.ANY)
    dma = pltpu.SemaphoreType.DMA
    bf16 = jnp.bfloat16
    table_rows = -(-(9 + 2 * planes) // 8) * 8
    full = (full_pair, full_plane)
    cos, sin = (jnp.asarray(table.reshape(turns, UNIT, HEAD)) for table in rotary_tables(prefix, rows))
    units = queries.reshape(held * turns, UNIT, width)
    base = [min(level[0] for level in levels)] * half
    base += [min(level[2] for level in levels)] * (planes - half - 1)
    base_shape = (len(base), pair, max(base), UNIT, wide)
    far_shape = jax.ShapeDtypeStruct((cached, prefix, HEAD), bf16)
    tables, chosen, k_far, v_far, q_base = pl.pallas_call(
        functools.partial(plan_kernel, groups, pair, levels, full, base),
        out_shape=[
            jax.ShapeDtypeStruct((table_rows, LANES), jnp.int32),
            jax.ShapeDtypeStruct((1,), jnp.int32),
            far_shape, far_shape,
            jax.ShapeDtypeStruct(base_shape, bf16),
        ],
        in_specs=[smem] * 3 + [vmem, anywhere, anywhere, vmem, vmem],
        out_specs=[vmem, smem] + [anywhere] * 3,
        scratch_shapes=[
            pltpu.VMEM((1, LANES), jnp.int32),
            pltpu.VMEM((groups, 1, LANES), jnp.int32),
            pltpu.VMEM(base_shape, bf16),
            dma((groups,)), dma((groups,)),
            dma((len(base), pair)), dma((len(base), pair)), dma((2,)), dma((2,)),
        ],
        compiler_params=pltpu.CompilerParams(collective_id=1, has_side_effects=True),
        name="plan_and_share",
    )(slot_of_prompt, prompt_of, lengths, units, prefix_keys, prefix_values, cos, sin)
    operands = (tables, units, prefix_keys, prefix_values, k_far, v_far, q_base, cos, sin)

    def branch(level):
        cap1, cap2, near1, near2, *batches = caps = levels[level]
        counts1 = [cap1] * half + [near1] * half
        counts2 = [cap2] * half + [near2] * half

        def run(*values):
            return pl.pallas_call(
                functools.partial(packed_kernel, groups, lanes, pair, full, caps, cuts, base),
                out_shape=jax.ShapeDtypeStruct((held * share, UNIT, width * lanes), bf16),
                in_specs=[smem, vmem] + [anywhere] * 5 + [vmem, vmem],
                out_specs=vmem,
                scratch_shapes=[
                    *(pltpu.VMEM((pair, count, UNIT, wide), bf16) for count in counts1),
                    *(pltpu.VMEM((half, pair, count, UNIT, wide), bf16) for count in (cap1, near1)),
                    *(pltpu.VMEM((count * BATCH, UNIT, wide), bf16) for count in batches),
                    *(pltpu.VMEM((sum(counts2), UNIT, cut), bf16) for cut in cuts),
                    *(pltpu.VMEM((sum(counts2), UNIT, cut), bf16) for cut in cuts),
                    *(pltpu.VMEM((pair, lanes, held * share, UNIT, cut), bf16) for cut in cuts),
                    pltpu.VMEM((slots, prefix, HEAD), bf16),
                    pltpu.VMEM((slots, prefix, HEAD), bf16),
                    dma((planes, pair)), dma((planes, pair)), dma((4,)), dma((len(base),)),
                    dma((PIECES, planes)), dma((PIECES, planes)),
                    dma((PIECES, pair, lanes)), dma((PIECES, pair, lanes)),
                ],
                compiler_params=pltpu.CompilerParams(
                    collective_id=2 + level, has_side_effects=True
                ),
                name=f"packed_prefix_attention_{level}",
            )(*values)

        return run

    out = lax.switch(
        chosen.reshape(()), [branch(level) for level in range(len(levels))], *operands
    )
    return out.reshape(held, share * UNIT, width * lanes)


def fits(groups, lanes, queries, prefix_keys):
    held, rows, width = queries.shape
    pair = prefix_keys.shape[2] // HEAD
    if pair != 2 or groups // pair not in (2, 4) or groups % (2 * pair):
        return False
    if rows % (UNIT * lanes) or rows >= LANES:
        return False
    slots = pair * prefix_keys.shape[0]
    spots = 2 * groups * prefix_keys.shape[0]
    full_plane = CAPC * pair * pair * rows // UNIT
    room = groups // pair // 2 * full_plane + slots * (BATCH - 1)
    return max(groups * held, spots, full_plane) <= LANES and room <= 2 * LANES


def local(groups, lanes, queries, prefix_keys, *rest):
    form = packed if fits(groups, lanes, queries, prefix_keys) else padded
    return form(groups, lanes, queries, prefix_keys, *rest)


def solution(mesh):
    placed = (
        P("group", None, "tensor"),
        P("group", None, "tensor"),
        P("group", None, "tensor"),
        P(),
        P("group"),
        P("group"),
    )
    return jax.shard_map(
        functools.partial(local, mesh.shape["group"], mesh.shape["tensor"]),
        mesh=mesh, in_specs=placed, out_specs=P("group", "tensor", None), check_vma=False,
    )
```

```python
import functools
import math

import numpy as np

import jax
import jax.numpy as jnp
from jax import lax
from jax.experimental import pallas as pl
from jax.experimental.pallas import tpu as pltpu
from jax.sharding import PartitionSpec as P

HEAD = 128
CAPC = 2
ROTARY_BASE = 1000000.0
TILE = 16
UNIT = 8
BATCH = 4
LANES = 128
MESH = pl.DeviceIdType.MESH
PIECES = 3
ROOM = 28 * 2**20
LEVELS = (
    (0.65625, 0.4375, 0.6875, 0.5625, 0.4286, 0.4286),
    (0.65625, 0.5, 0.75, 0.59375, 0.4571, 0.4571),
    (0.65625, 0.5625, 0.75, 0.625, 0.4857, 0.4857),
    (0.75, 0.5, 0.8125, 0.625, 0.4857, 0.4857),
    (0.75, 0.5625, 0.875, 0.6875, 0.5143, 0.5143),
    (0.84375, 0.65625, 0.9375, 0.75, 0.5429, 0.5429),
    (1, 1, 1, 1, 1.0000, 1.0000),
)


def rotary_tables(first_position, rows):
    half = HEAD // 2
    frequencies = np.float32(ROTARY_BASE) ** (
        -(np.arange(half, dtype=np.float32) * np.float32(2.0) / np.float32(HEAD))
    )
    positions = (first_position + np.arange(rows)).astype(np.float32)
    angles = (positions[:, None] * frequencies.astype(np.float32)[None, :]).astype(np.float64)
    cos, sin = np.cos(angles), np.sin(angles)
    return (
        np.concatenate([cos, cos], axis=1).astype(np.float32),
        np.concatenate([-sin, sin], axis=1).astype(np.float32),
    )


def padded_kernel(
    groups, lanes, moved,
    source_ref, tag_ref, dest_ref, length_ref,
    q_ref, k_ref, v_ref, cos_ref, sin_ref,
    out_ref,
    q_out, q_in, sel_out, sel_in, res, stage,
    q_send, q_recv, s_send, s_recv, r_send, r_recv,
    *near,
):
    me, lane = lax.axis_index("group"), lax.axis_index("tensor")
    held, rows, width = q_ref.shape
    cached, prefix, kv_width = k_ref.shape
    share = rows // lanes
    kv_local = kv_width // HEAD
    per_kv = width // HEAD // kv_local
    half = groups // 2
    factor = math.log2(math.e) / math.sqrt(HEAD)
    wide_near = moved * per_kv * HEAD
    if moved:
        (n_out, n_in, ns_out, ns_in, n_res, k_far, v_far,
         n_send, n_recv, ns_send, ns_recv, nr_send, nr_recv, kv_send, kv_recv) = near
    spot = lax.rem(me, half)
    base = me - spot
    mirror = lax.rem(me + half, groups)

    barrier = pltpu.get_barrier_semaphore()

    def greet(step, carry):
        for turn in range(lanes):
            def send():
                pl.semaphore_signal(
                    barrier, inc=1,
                    device_id=(lax.rem(me + step, groups), lax.rem(lane + turn, lanes)),
                    device_id_type=MESH,
                )
            if turn:
                send()
            else:
                pl.when(step > 0)(send)
        return carry

    lax.fori_loop(0, groups, greet, 0)

    def offset_of(step):
        swing = (step + 1) // 2
        return lax.rem(half + (1 - 2 * lax.rem(step, 2)) * swing + groups, groups)

    def route(owner):
        places = [owner * CAPC + slot for slot in range(CAPC)]
        return [(source_ref[place], tag_ref[place]) for place in places]

    def fill(items, q_to, sel_to, block, first, last):
        for slot, (item, tag) in enumerate(items):
            for j in range(cached):
                weight = jnp.where(tag == j, 1.0, 0.0)
                sel_to[block, slot * cached + j] = jnp.full(
                    (TILE, HEAD), weight, jnp.float32
                ).astype(jnp.bfloat16)
            for head in range(first, last):
                x = q_ref[item, :, head * HEAD:(head + 1) * HEAD].astype(jnp.float32)
                turned = x * cos_ref[...] + pltpu.roll(x, HEAD // 2, 1) * sin_ref[...]
                span = slice((head - first) * HEAD, (head - first + 1) * HEAD)
                q_to[block, slot, :, span] = turned.astype(jnp.bfloat16)

    near_heads, all_heads = moved * per_kv, width // HEAD

    def pair(src, dst, send_sem, recv_sem, device):
        return pltpu.make_async_remote_copy(
            src_ref=src, dst_ref=dst, send_sem=send_sem, recv_sem=recv_sem,
            device_id=device, device_id_type=MESH,
        )

    def q_copies(here, there, device):
        return (
            pair(sel_out.at[here], sel_in.at[there], s_send.at[here], s_recv.at[there],
                 (device, lane)),
            pair(q_out.at[here], q_in.at[there], q_send.at[here], q_recv.at[there],
                 (device, lane)),
        )

    def n_copies(here, there, device):
        return (
            pair(ns_out.at[here], ns_in.at[there], ns_send.at[here], ns_recv.at[there],
                 (device, lane)),
            pair(n_out.at[here], n_in.at[there], n_send.at[here], n_recv.at[there],
                 (device, lane)),
        )

    def place(owner, from_lane, skip, wide):
        start = pl.multiple_of(from_lane * width + skip, HEAD)
        return stage.at[pl.ds(owner * CAPC, CAPC), :, pl.ds(start, wide)]

    def r_copy(block, piece, owner, from_lane, device):
        return pair(
            res.at[block, :, piece], place(owner, from_lane, wide_near, width - wide_near),
            r_send.at[block, piece], r_recv.at[owner, from_lane], (device, piece),
        )

    def nr_copy(block, piece, owner, from_lane, device):
        return pair(
            n_res.at[block, :, piece], place(owner, from_lane, 0, wide_near),
            nr_send.at[block, piece], nr_recv.at[owner, from_lane], (device, piece),
        )

    def kv_copies():
        span = pl.ds(0, moved * HEAD)
        return (
            pair(k_ref.at[:, :, span], k_far, kv_send.at[0], kv_recv.at[0], (mirror, lane)),
            pair(v_ref.at[:, :, span], v_far, kv_send.at[1], kv_recv.at[1], (mirror, lane)),
        )

    items = route(mirror)
    fill(items, q_out, sel_out, mirror, near_heads, all_heads)
    pl.semaphore_wait(barrier, groups * lanes - 1)
    for copy in q_copies(mirror, me, mirror):
        copy.start()
    if moved:
        fill(items, n_in, ns_in, spot + half, 0, near_heads)

    def dispatch(step, carry):
        owner = lax.rem(me + offset_of(step), groups)
        items = route(owner)
        fill(items, q_out, sel_out, owner, near_heads, all_heads)
        for copy in q_copies(owner, me, owner):
            copy.start()
        if moved:
            fill(items, n_out, ns_out, owner, 0, near_heads)
            seat = lax.rem(owner, half)
            kind = lax.rem(lax.div(owner, half) + lax.div(me, half), 2)
            for copy in n_copies(owner, spot + half * kind, base + seat):
                copy.start()
        return carry

    lax.fori_loop(1, groups - 1, dispatch, 0)
    if moved:
        for copy in kv_copies():
            copy.start()
    items = route(me)
    fill(items, q_in, sel_in, me, near_heads, all_heads)
    if moved:
        fill(items, n_in, ns_in, spot, 0, near_heads)

    def attend(q_from, sel_from, to, block, keys, values, first, count):
        for slot in range(CAPC):
            weights = [sel_from[block, slot * cached + j][None] for j in range(cached)]

            def chosen(ref, span):
                total = None
                for j in range(cached):
                    part = ref[j, :, span].reshape(prefix // TILE, TILE, HEAD) * weights[j]
                    total = part if total is None else total + part
                return total.reshape(prefix, HEAD)

            for kv in range(count):
                span = slice((first + kv) * HEAD, (first + kv + 1) * HEAD)
                spans = [
                    slice((kv * per_kv + g) * HEAD, (kv * per_kv + g + 1) * HEAD)
                    for g in range(per_kv)
                ]
                query = jnp.concatenate([q_from[block, slot, :, s] for s in spans], axis=0)
                scores = lax.dot_general(
                    query, chosen(keys, span), (((1,), (1,)), ((), ())),
                    preferred_element_type=jnp.float32,
                )
                peak = jnp.max(scores, axis=-1, keepdims=True)
                weight = jnp.exp2((scores - peak) * factor)
                total = jnp.sum(weight, axis=-1, keepdims=True)
                mixed = jnp.dot(
                    weight.astype(jnp.bfloat16), chosen(values, span),
                    preferred_element_type=jnp.float32,
                )
                mixed = (mixed / total).astype(jnp.bfloat16)
                for g in range(per_kv):
                    to[block, slot, :, :, spans[g]] = mixed[g * rows:(g + 1) * rows].reshape(
                        lanes, share, HEAD
                    )

    def give_back(step, copy, source, block, owner, done, skip, wide):
        for turn in range(1, lanes):
            copy(block, lax.rem(lane + turn, lanes), owner, lane, source).start()

        @pl.when(step > 0)
        def _():
            copy(block, lane, owner, lane, source).start()

        @pl.when(step == 0)
        def _():
            start = pl.multiple_of(lane * width + skip, HEAD)
            stage[pl.ds(owner * CAPC, CAPC), :, pl.ds(start, wide)] = done[block, :, lane]

    def far_work(step, carry):
        source = lax.rem(me + groups - offset_of(lax.rem(step + groups - 1, groups)), groups)

        @pl.when(step > 0)
        def _():
            for copy in q_copies(source, source, source):
                copy.wait_recv()

        attend(q_in, sel_in, res, source, k_ref, v_ref, moved, kv_local - moved)
        give_back(step, r_copy, source, source, me, res, wide_near, width - wide_near)
        return carry

    def near_work(kind, keys, values, owner):
        def body(step, carry):
            seat = lax.rem(spot + step, half)
            block = seat + half * kind

            @pl.when(step > 0)
            def _():
                for copy in n_copies(block, block, base + seat):
                    copy.wait_recv()

            attend(n_in, ns_in, n_res, block, keys, values, 0, moved)
            give_back(step, nr_copy, base + seat, block, owner, n_res, 0, wide_near)
            return carry

        lax.fori_loop(0, half, body, 0)

    if moved:
        near_work(0, k_ref, v_ref, me)
    lax.fori_loop(0, groups, far_work, 0)
    if moved:
        for copy in kv_copies():
            copy.wait_recv()
        near_work(1, k_far, v_far, mirror)

    def returned(step, copy, block, owner, device):
        @pl.when(step > 0)
        def _():
            copy(block, lane, owner, lane, device).wait_send()
            copy(block, lane, owner, lane, device).wait_recv()

        for turn in range(1, lanes):
            piece = lax.rem(lane + turn, lanes)
            copy(block, piece, owner, piece, device).wait_send()
            copy(block, piece, owner, piece, device).wait_recv()

    def far_settle(step, carry):
        other = lax.rem(me + step, groups)

        @pl.when(step > 0)
        def _():
            for copy in q_copies(other, me, other):
                copy.wait_send()

        returned(step, r_copy, other, other, other)
        return carry

    lax.fori_loop(0, groups, far_settle, 0)
    if moved:
        for copy in kv_copies():
            copy.wait_send()

        def near_settle(step, carry):
            seat = lax.rem(spot + step, half)
            for kind in range(2):
                owner = lax.rem(base + half * kind, groups) + seat

                @pl.when(step > 0)
                def _():
                    for copy in n_copies(owner, owner, base + seat):
                        copy.wait_send()

                returned(step, nr_copy, seat + half * kind, owner, base + seat)
            return carry

        lax.fori_loop(0, half, near_settle, 0)

    def deliver(item, carry):
        found = stage[dest_ref[item]].astype(jnp.float32)
        position = lane * share + lax.broadcasted_iota(jnp.int32, found.shape, 0)
        out_ref[item] = jnp.where(position < length_ref[item], found, 0.0).astype(jnp.bfloat16)
        return carry

    lax.fori_loop(0, held, deliver, 0)


def padded(groups, lanes, queries, prefix_keys, prefix_values, slot_of_prompt, prompt_of, lengths):
    held, rows, width = queries.shape
    cached, prefix, kv_width = prefix_keys.shape
    share = rows // lanes
    kv_local = kv_width // HEAD
    moved = kv_local // 2 if groups % 2 == 0 and groups >= 4 else 0
    wide_near = moved * (width // kv_local)
    wide = width - wide_near
    cos, sin = rotary_tables(prefix, rows)
    cache_rows = slot_of_prompt[prompt_of]
    owner = cache_rows // cached
    serial = jnp.arange(held)
    earlier = (owner[None, :] == owner[:, None]) & (serial[None, :] < serial[:, None])
    destination = owner * CAPC + jnp.sum(earlier.astype(jnp.int32), axis=1)
    matches = destination[None, :] == jnp.arange(groups * CAPC)[:, None]
    source = jnp.sum(jnp.where(matches, serial[None, :], 0), axis=1)
    tags = jnp.sum(jnp.where(matches, (cache_rows % cached)[None, :], 0), axis=1)
    smem = pl.BlockSpec(memory_space=pltpu.SMEM)
    vmem = pl.BlockSpec(memory_space=pltpu.VMEM)
    dma = pltpu.SemaphoreType.DMA
    bf16 = jnp.bfloat16

    def exchange(features):
        return [
            pltpu.VMEM((groups, CAPC, rows, features), bf16),
            pltpu.VMEM((groups, CAPC, rows, features), bf16),
            pltpu.VMEM((groups, CAPC * cached, TILE, HEAD), bf16),
            pltpu.VMEM((groups, CAPC * cached, TILE, HEAD), bf16),
            pltpu.VMEM((groups, CAPC, lanes, share, features), bf16),
        ]

    semaphores = [
        dma((groups,)), dma((groups,)),
        dma((groups,)), dma((groups,)),
        dma((groups, lanes)), dma((groups, lanes)),
    ]
    scratch = [
        *exchange(wide),
        pltpu.VMEM((groups * CAPC, share, width * lanes), bf16),
        *semaphores,
    ]
    if moved:
        scratch += [
            *exchange(wide_near),
            pltpu.VMEM((cached, prefix, moved * HEAD), bf16),
            pltpu.VMEM((cached, prefix, moved * HEAD), bf16),
            *semaphores,
            dma((2,)), dma((2,)),
        ]
    return pl.pallas_call(
        functools.partial(padded_kernel, groups, lanes, moved),
        out_shape=jax.ShapeDtypeStruct((held, share, width * lanes), bf16),
        in_specs=[smem] * 4 + [vmem] * 5,
        out_specs=vmem,
        scratch_shapes=scratch,
        compiler_params=pltpu.CompilerParams(collective_id=0, has_side_effects=True),
        name="routed_prefix_attention",
    )(
        source.astype(jnp.int32), tags.astype(jnp.int32), destination.astype(jnp.int32), lengths,
        queries, prefix_keys, prefix_values, jnp.asarray(cos), jnp.asarray(sin),
    )


def xor_order(step, plane, planes):
    half = planes // 2
    near = lax.div(step, half)
    side = lax.rem(lax.div(plane, half) + 1 - near, 2)
    return side * half + lax.rem(lax.rem(plane, half) + step + near, half)


def step_of(plane, z, planes):
    half = planes // 2
    shift = lax.rem(plane + planes - z, half)
    far = shift
    near = half + lax.rem(shift + half - 1, half)
    return jnp.where(plane // half != z // half, far, near)


def plan_kernel(
    groups, pair, levels, full, base,
    slot_ref, prompt_ref, length_ref, q_ref, k_ref, v_ref, cos_ref, sin_ref,
    tables_ref, level_ref, k_far, v_far, q_base,
    mine, gathered, q_out, send, recv, q_send, q_recv, kv_send, kv_recv,
):
    shared = len(base)
    me, lane = lax.axis_index("group"), lax.axis_index("tensor")
    held = prompt_ref.shape[0]
    slots = slot_ref.shape[0]
    planes = groups // pair
    per_plane = slots // planes
    total = groups * held
    full_pair, full_plane = full
    turns = full_pair // (CAPC * pair)
    half = planes // 2
    z, x = lax.div(me, pair), lax.rem(me, pair)
    partner = z * pair + 1 - x
    there = [xor_order(step, z, planes) for step in range(shared)]
    barrier = pltpu.get_barrier_semaphore()

    def greet(step, carry):
        pl.semaphore_signal(
            barrier, inc=1, device_id=(lax.rem(me + step, groups), lane), device_id_type=MESH
        )
        return carry

    lax.fori_loop(1, groups, greet, 0)

    def remote(src, dst, send_sem, recv_sem, group):
        return pltpu.make_async_remote_copy(
            src_ref=src, dst_ref=dst, send_sem=send_sem, recv_sem=recv_sem,
            device_id=(group, lane), device_id_type=MESH,
        )

    span = pl.ds(pl.multiple_of((1 - x) * HEAD, HEAD), HEAD)
    kv_copies = [
        remote(ref.at[:, :, span], far_ref, kv_send.at[i], kv_recv.at[i], partner)
        for i, (ref, far_ref) in enumerate(((k_ref, k_far), (v_ref, v_far)))
    ]

    def q_copy(step, j, source, device):
        return remote(
            q_out.at[step, j, pl.ds(0, base[step])], q_base.at[step, source, pl.ds(0, base[step])],
            q_send.at[step, j], q_recv.at[step, source], device,
        )

    own_slots = [slot_ref[prompt_ref[i]] for i in range(held)]
    own_planes = [lax.div(slot, per_plane) for slot in own_slots]
    own_counts = [lax.div(length_ref[i] + UNIT - 1, UNIT) for i in range(held)]
    own_starts = []
    for i in range(held):
        start = jnp.int32(0)
        for other in range(i):
            start = start + jnp.where(own_planes[other] == own_planes[i], own_counts[other], 0)
        own_starts.append(start)

    def fill(step):
        starts = [
            jnp.where(own_planes[i] == there[step], own_starts[i], LANES) for i in range(held)
        ]

        def one(k, carry):
            index = jnp.int32(0)
            for i in range(held):
                offset = k - starts[i]
                hit = (offset >= 0) & (offset < own_counts[i])
                index = index + jnp.where(hit, i * turns + offset, 0)
            rope(index, q_ref, cos_ref, sin_ref, q_out.at[step], k, pair)
            return carry

        lax.fori_loop(0, base[step], one, 0)

    lanes1 = lax.broadcasted_iota(jnp.int32, (1, LANES), 1)
    row = jnp.zeros((1, LANES), jnp.int32)
    for i in range(held):
        value = own_slots[i] * LANES + length_ref[i]
        row = jnp.where(lanes1 == me * held + i, value, row)
    mine[...] = row
    gathered[me] = row
    for step in range(half):
        fill(step)
    pl.semaphore_wait(barrier, groups - 1)

    def copy(there, device):
        return pltpu.make_async_remote_copy(
            src_ref=mine, dst_ref=gathered.at[there], send_sem=send.at[device],
            recv_sem=recv.at[there], device_id=(device, lane), device_id_type=MESH,
        )

    def push(step, carry):
        copy(me, lax.rem(me + step, groups)).start()
        return carry

    lax.fori_loop(1, groups, push, 0)

    def dispatch(step):
        for j in range(pair):
            q_copy(step, j, x, there[step] * pair + j).start()

    for step in range(half):
        dispatch(step)
    for kv_copy in kv_copies:
        kv_copy.start()
    for step in range(half, shared):
        fill(step)
        dispatch(step)

    def settle(step, carry):
        other = lax.rem(me + step, groups)
        copy(other, other).wait_recv()
        copy(me, other).wait_send()
        return carry

    lax.fori_loop(1, groups, settle, 0)
    code = gathered[0]
    for g in range(1, groups):
        code = code + gathered[g]

    square = (LANES, LANES)
    down = lax.broadcasted_iota(jnp.int32, square, 0)
    across = lax.broadcasted_iota(jnp.int32, square, 1)
    eye = down == across

    def to_column(values):
        return jnp.sum(jnp.where(eye, jnp.broadcast_to(values, square), 0), axis=1, keepdims=True)

    def to_row(values):
        return jnp.sum(jnp.where(eye, jnp.broadcast_to(values, square), 0), axis=0, keepdims=True)

    def facts(values, index):
        live = index < total
        length = values % LANES
        slot = values // LANES
        count = jnp.where(live, (length + UNIT - 1) // UNIT, 0)
        return count, slot, slot // per_plane, index // held, index // (held * pair)

    col = to_column(code)
    down1 = lax.broadcasted_iota(jnp.int32, (LANES, 1), 0)
    count_r, slot_r, to_r, from_r, plane_r = facts(code, lanes1)
    count_c, slot_c, to_c, from_c, plane_c = facts(col, down1)
    weight = jnp.broadcast_to(count_c, square)
    earlier = (down < across) & (to_c == to_r)

    def rank(mask):
        return jnp.sum(jnp.where(mask, weight, 0), axis=0, keepdims=True)

    base1 = rank(earlier & (from_c == from_r))
    base2 = rank(earlier & (plane_c == plane_r))
    side_r = jnp.where(plane_r // half == to_r // half, 1, 0)
    side_c = jnp.where(plane_c // half == to_c // half, 1, 0)
    within = rank(earlier & (side_c == side_r) & (slot_c == slot_r))
    key_r = side_r * slots + slot_r
    number = jnp.sum(
        jnp.where(down1 == key_r, jnp.broadcast_to(count_r, square), 0), axis=1, keepdims=True
    )
    need = (number + BATCH - 1) // BATCH
    need_r = to_row(need)
    first = jnp.sum(
        jnp.where(
            (down // per_plane == across // per_plane) & (across < down),
            jnp.broadcast_to(need_r, square), 0,
        ),
        axis=1, keepdims=True,
    )
    first_of = jnp.sum(
        jnp.where(down1 == key_r, jnp.broadcast_to(first, square), 0), axis=0, keepdims=True
    )
    place = first_of * BATCH + within
    base1_c, base2_c, place_c = to_column(base1), to_column(base2), to_column(place)

    alive = lanes1 < total
    far = alive & (to_r // half != plane_r // half)
    near = alive & (to_r // half == plane_r // half)
    needs = [
        jnp.max(jnp.where(mask, begin + count_r, 0))
        for mask in (far, near) for begin in (base1, base2)
    ] + [jnp.max(jnp.where(down1 // slots == side, first + need, 0)) for side in range(2)]
    level = jnp.int32(len(levels) - 1)
    for index, caps in reversed(list(enumerate(levels[:-1]))):
        over = needs[0] > caps[0]
        for value, cap in zip(needs[1:], caps[1:]):
            over = over | (value > cap)
        level = jnp.where(over, level, index)
    level_ref[0] = level
    tables_ref[pl.ds(1, 1), :] = code
    tables_ref[pl.ds(2, 1), :] = step_of(to_r, z, planes) * full_plane + base2

    def pick(mask, start_c, value_c, index):
        hit = mask & (index >= start_c) & (index < start_c + count_c)
        return jnp.sum(jnp.where(hit, value_c + index, 0), axis=0, keepdims=True)

    for plane in range(planes):
        tables_ref[pl.ds(3 + plane, 1), :] = pick(
            (from_c == me) & (to_c == plane), base1_c,
            lax.rem(down1, held) * turns - base1_c, lanes1,
        )
        tables_ref[pl.ds(3 + planes + plane, 1), :] = pick(
            (plane_c == plane) & (to_c == z), base2_c, place_c - base2_c, lanes1
        )
    seat_c = lax.rem(step_of(plane_c, z, planes), half) * pair + lax.rem(from_c, pair)
    for side in range(2):
        for page in range(2):
            tables_ref[pl.ds(3 + 2 * planes + 2 * side + page, 1), :] = pick(
                (side_c == side) & (to_c == z), place_c,
                seat_c * full_pair + base1_c - place_c, lanes1 + page * LANES,
            )
        starts = (
            (down1 // slots == side) & (lax.rem(down1, slots) // per_plane == z)
            & (lanes1 >= first) & (lanes1 < first + need)
        )
        tables_ref[pl.ds(7 + 2 * planes + side, 1), :] = jnp.sum(
            jnp.where(starts, lax.rem(down1, per_plane), 0), axis=0, keepdims=True
        )
    for step in range(shared):
        for j in range(pair):
            q_copy(step, j, j, me).wait_recv()
            q_copy(step, j, x, there[step] * pair + j).wait_send()
    for kv_copy in kv_copies:
        kv_copy.wait_recv()
        kv_copy.wait_send()


def rope(index, q_ref, cos_ref, sin_ref, to, k, pair):
    turn = lax.rem(index, cos_ref.shape[0])
    cos, sin = cos_ref[turn], sin_ref[turn]
    block = q_ref[index].astype(jnp.float32)
    per_kv = block.shape[-1] // HEAD // pair
    for j in range(pair):
        parts = []
        for g in range(per_kv):
            head = j * per_kv + g
            part = block[:, head * HEAD:(head + 1) * HEAD]
            turned = part * cos + pltpu.roll(part, HEAD // 2, 1) * sin
            parts.append(turned.astype(jnp.bfloat16))
        to[j, k] = jnp.concatenate(parts, axis=1)


def packed_kernel(
    groups, lanes, pair, full, caps, cuts, base,
    tables,
    q_ref, k_ref, v_ref, k_far, v_far, q_base, cos_ref, sin_ref,
    out_ref,
    *scratch,
):
    me, lane = lax.axis_index("group"), lax.axis_index("tensor")
    planes = groups // pair
    half = planes // 2
    pieces = len(cuts)
    scratch = list(scratch)

    def take(count):
        taken = scratch[:count]
        del scratch[:count]
        return taken

    q_out, q_sides, results = take(planes), take(2), take(2)
    q_in = [q_sides[step // half].at[step % half] for step in range(planes)]
    r_out, r_in, stage = take(pieces), take(pieces), take(pieces)
    k_all, v_all = take(2)
    q_send, q_recv, kv_here, q_here, r_send, r_recv, f_send, f_recv = scratch

    z, x = lax.div(me, pair), lax.rem(me, pair)
    cached, prefix, _ = k_ref.shape
    units, _, width = q_ref.shape
    wide = width // pair
    per_kv = wide // HEAD
    turns = cos_ref.shape[0]
    held = units // turns
    share = turns // lanes
    full_pair, full_plane = full
    cap1, cap2, near1, near2 = caps[:4]
    factor = math.log2(math.e) / math.sqrt(HEAD)
    send_row, ret_row, comp_row, slot_row = 3, 3 + planes, 3 + 2 * planes, 7 + 2 * planes
    counts1 = [cap1 if step < half else near1 for step in range(planes)]
    counts2 = [cap2 if step < half else near2 for step in range(planes)]
    offsets = [sum(counts2[:step]) for step in range(planes)]
    last = planes - 1
    there = [xor_order(step, z, planes) for step in range(planes)]

    barrier = pltpu.get_barrier_semaphore()

    def greet(step, carry):
        pl.semaphore_signal(
            barrier, inc=1, device_id=(lax.rem(me + step, groups), lane), device_id_type=MESH
        )
        return carry

    lax.fori_loop(1, groups, greet, 0)
    for turn in range(1, lanes):
        for j in range(pair):
            pl.semaphore_signal(
                barrier, inc=1,
                device_id=(z * pair + j, lax.rem(lane + turn, lanes)), device_id_type=MESH,
            )

    def span_of(j):
        return pl.ds(pl.multiple_of(j * HEAD, HEAD), HEAD)

    here = [
        pltpu.make_async_copy(
            ref.at[:, :, span_of(x)], full_ref.at[pl.ds(x * cached, cached)], kv_here.at[i]
        )
        for i, (ref, full_ref) in enumerate(((k_ref, k_all), (v_ref, v_all)))
    ] + [
        pltpu.make_async_copy(
            far_ref, full_ref.at[pl.ds((1 - x) * cached, cached)], kv_here.at[2 + i]
        )
        for i, (far_ref, full_ref) in enumerate(((k_far, k_all), (v_far, v_all)))
    ] + [
        pltpu.make_async_copy(
            q_base.at[step, :, pl.ds(0, base[step])], q_in[step].at[:, pl.ds(0, base[step])],
            q_here.at[step],
        )
        for step in range(len(base))
    ]
    for copy in here:
        copy.start()

    def remote(src, dst, send_sem, recv_sem, group, to_lane):
        return pltpu.make_async_remote_copy(
            src_ref=src, dst_ref=dst, send_sem=send_sem, recv_sem=recv_sem,
            device_id=(group, to_lane), device_id_type=MESH,
        )

    rest = [
        slice(base[step] if step < len(base) else 0, counts1[step]) for step in range(planes)
    ]

    def q_copy(step, j, source, device):
        span = pl.ds(rest[step].start, rest[step].stop - rest[step].start)
        return remote(
            q_out[step].at[j, span], q_in[step].at[source, span], q_send.at[step, j],
            q_recv.at[step, source], device, lane,
        )

    def fill(step):
        def one(k, carry):
            index = tables[send_row + there[step], k]
            rope(index, q_ref, cos_ref, sin_ref, q_out[step], k, pair)
            return carry

        lax.fori_loop(rest[step].start, rest[step].stop, one, 0)

    moving = [step for step in range(planes) if rest[step].stop > rest[step].start]

    def dispatch(step):
        if step not in moving:
            return
        for j in range(pair):
            if step < last:
                q_copy(step, j, x, there[step] * pair + j).start()
            else:
                @pl.when(j != x)
                def _():
                    q_copy(step, j, x, there[step] * pair + j).start()

    for step in moving:
        fill(step)
    q_in[last][x] = q_out[last][x]

    def greeted():
        pl.semaphore_wait(barrier, groups - 1 + pair * (lanes - 1))
        for step in moving:
            dispatch(step)

    if 0 in moving:
        greeted()
    for copy in here:
        copy.wait()

    def r_copy(piece, step):
        region = pl.ds(offsets[step], counts2[step])
        return remote(
            r_out[piece].at[region], r_in[piece].at[region],
            r_send.at[piece, step], r_recv.at[piece, step], there[step] * pair + x, lane,
        )

    for side in range(2):
        steps = range(side * half, side * half + half)
        for step in steps:
            for j in range(pair) if step in moving else []:
                if step < last:
                    q_copy(step, j, j, me).wait_recv()
                else:
                    @pl.when(j != x)
                    def _():
                        q_copy(step, j, j, me).wait_recv()

        def batch(b, carry):
            slot = tables[slot_row + side, b]
            blocks = []
            for i in range(BATCH):
                entry = b * BATCH + i
                index = tables[
                    comp_row + 2 * side + lax.div(entry, LANES), lax.rem(entry, LANES)
                ]
                seat = lax.div(index, full_pair)
                blocks.append(
                    q_sides[side][
                        lax.div(seat, pair), lax.rem(seat, pair), lax.rem(index, full_pair)
                    ].astype(jnp.float32)
                )
            query = jnp.concatenate(
                [block[:, g * HEAD:(g + 1) * HEAD] for g in range(per_kv) for block in blocks],
                axis=0,
            ).astype(jnp.bfloat16)
            scores = lax.dot_general(
                query, k_all[slot], (((1,), (1,)), ((), ())), preferred_element_type=jnp.float32
            )
            peak = jnp.max(scores, axis=-1, keepdims=True)
            weight = jnp.exp2((scores - peak) * factor)
            total = jnp.sum(weight, axis=-1, keepdims=True)
            mixed = jnp.dot(
                weight.astype(jnp.bfloat16), v_all[slot], preferred_element_type=jnp.float32
            ) / total
            for i in range(BATCH):
                results[side][b * BATCH + i] = jnp.concatenate(
                    [
                        mixed[(g * BATCH + i) * UNIT:(g * BATCH + i + 1) * UNIT]
                        for g in range(per_kv)
                    ],
                    axis=1,
                ).astype(jnp.bfloat16)
            return carry

        lax.fori_loop(0, results[side].shape[0] // BATCH, batch, 0, unroll=2)
        if side == 0 and 0 not in moving:
            greeted()
        for step in steps:
            target = r_out if step < last else r_in

            def pack(k, carry):
                found = results[side][tables[ret_row + there[step], k]]
                start = 0
                for piece in range(pieces):
                    target[piece][offsets[step] + k] = found[:, start:start + cuts[piece]]
                    start += cuts[piece]
                return carry

            lax.fori_loop(0, counts2[step], pack, 0, unroll=2)
            if step < last:
                r_copy(0, step).start()
            if step == half - 1:
                for piece in range(1, pieces):
                    for ready in range(half):
                        r_copy(piece, ready).start()
            if step == last - 1:
                for piece in range(1, pieces):
                    for ready in range(half, last):
                        r_copy(piece, ready).start()

    def lineup(step):
        return lax.rem(x + step + 1, pair), lax.rem(lane + lax.div(step + 1, pair), lanes)

    def final(piece, at_x, at_lane, from_x, from_lane, to_x, to_lane):
        skip = sum(cuts[:piece])
        start = pl.multiple_of((from_lane * pair + from_x) * wide + skip, HEAD)
        return remote(
            stage[piece].at[at_x, at_lane], out_ref.at[:, :, pl.ds(start, cuts[piece])],
            f_send.at[piece, at_x, at_lane], f_recv.at[piece, from_x, from_lane],
            z * pair + to_x, to_lane,
        )

    for piece in range(pieces):
        for step in range(last):
            r_copy(piece, step).wait_recv()

        def spread(step, carry):
            to_x, to_lane = lineup(step)

            def one(i, inner):
                item = (z * pair + to_x) * held + i
                entry = tables[2, item]
                length = lax.rem(tables[1, item], LANES)
                source, rank = lax.div(entry, full_plane), lax.rem(entry, full_plane)
                cap = jnp.where(source < half, cap2, near2)
                offset = jnp.where(
                    source < half, source * cap2, half * cap2 + (source - half) * near2
                )
                for s in range(share):
                    unit = to_lane * share + s
                    found = r_in[piece][offset + jnp.minimum(rank + unit, cap - 1)].astype(
                        jnp.float32
                    )
                    row = unit * UNIT + lax.broadcasted_iota(jnp.int32, found.shape, 0)
                    stage[piece][to_x, to_lane, i * share + s] = jnp.where(
                        row < length, found, 0.0
                    ).astype(jnp.bfloat16)
                return inner

            lax.fori_loop(0, held, one, 0, unroll=2)

            @pl.when(step < pair * lanes - 1)
            def _():
                final(piece, to_x, to_lane, x, lane, to_x, to_lane).start()
            return carry

        lax.fori_loop(0, pair * lanes, spread, 0)
        start = pl.multiple_of((lane * pair + x) * wide + sum(cuts[:piece]), HEAD)
        out_ref[:, :, pl.ds(start, cuts[piece])] = stage[piece][x, lane]

    def drain(step, carry):
        to_x, to_lane = lineup(step)
        for piece in range(pieces):
            final(piece, to_x, to_lane, to_x, to_lane, to_x, to_lane).wait_recv()
            final(piece, to_x, to_lane, x, lane, to_x, to_lane).wait_send()
        return carry

    lax.fori_loop(0, pair * lanes - 1, drain, 0)
    for step in range(planes):
        for j in range(pair) if step in moving else []:
            if step < last:
                q_copy(step, j, x, there[step] * pair + j).wait_send()
            else:
                @pl.when(j != x)
                def _():
                    q_copy(step, j, x, there[step] * pair + j).wait_send()
        if step < last:
            for piece in range(pieces):
                r_copy(piece, step).wait_send()


def packed(groups, lanes, queries, prefix_keys, prefix_values, slot_of_prompt, prompt_of, lengths):
    held, rows, width = queries.shape
    cached, prefix, kv_width = prefix_keys.shape
    pair = kv_width // HEAD
    planes = groups // pair
    half = planes // 2
    turns = rows // UNIT
    full_pair = CAPC * pair * turns
    full_plane = full_pair * pair
    slots = cached * pair
    full_side = (full_plane * half + slots * (BATCH - 1)) // BATCH
    share = turns // lanes
    wide = width // pair
    per_kv = wide // HEAD
    cuts = [HEAD * (per_kv // PIECES + (i < per_kv % PIECES)) for i in range(PIECES)]
    levels = [
        tuple(
            round(whole * part)
            for whole, part in zip((full_pair, full_plane) * 2 + (full_side, full_side), level)
        )
        for level in LEVELS
    ]
    smem = pl.BlockSpec(memory_space=pltpu.SMEM)
    vmem = pl.BlockSpec(memory_space=pltpu.VMEM)
    anywhere = pl.BlockSpec(memory_space=pl.ANY)
    dma = pltpu.SemaphoreType.DMA
    bf16 = jnp.bfloat16
    table_rows = -(-(9 + 2 * planes) // 8) * 8
    full = (full_pair, full_plane)
    cos, sin = (jnp.asarray(table.reshape(turns, UNIT, HEAD)) for table in rotary_tables(prefix, rows))
    units = queries.reshape(held * turns, UNIT, width)
    base = [min(level[0] for level in levels)] * half
    base += [min(level[2] for level in levels)] * (planes - half - 1)
    base_shape = (len(base), pair, max(base), UNIT, wide)
    far_shape = jax.ShapeDtypeStruct((cached, prefix, HEAD), bf16)
    tables, chosen, k_far, v_far, q_base = pl.pallas_call(
        functools.partial(plan_kernel, groups, pair, levels, full, base),
        out_shape=[
            jax.ShapeDtypeStruct((table_rows, LANES), jnp.int32),
            jax.ShapeDtypeStruct((1,), jnp.int32),
            far_shape, far_shape,
            jax.ShapeDtypeStruct(base_shape, bf16),
        ],
        in_specs=[smem] * 3 + [vmem, anywhere, anywhere, vmem, vmem],
        out_specs=[vmem, smem] + [anywhere] * 3,
        scratch_shapes=[
            pltpu.VMEM((1, LANES), jnp.int32),
            pltpu.VMEM((groups, 1, LANES), jnp.int32),
            pltpu.VMEM(base_shape, bf16),
            dma((groups,)), dma((groups,)),
            dma((len(base), pair)), dma((len(base), pair)), dma((2,)), dma((2,)),
        ],
        compiler_params=pltpu.CompilerParams(
            collective_id=1, has_side_effects=True, vmem_limit_bytes=ROOM
        ),
        name="plan_and_share",
    )(slot_of_prompt, prompt_of, lengths, units, prefix_keys, prefix_values, cos, sin)
    operands = (tables, units, prefix_keys, prefix_values, k_far, v_far, q_base, cos, sin)

    def branch(level):
        cap1, cap2, near1, near2, *batches = caps = levels[level]
        counts1 = [cap1] * half + [near1] * half
        counts2 = [cap2] * half + [near2] * half

        def run(*values):
            return pl.pallas_call(
                functools.partial(packed_kernel, groups, lanes, pair, full, caps, cuts, base),
                out_shape=jax.ShapeDtypeStruct((held * share, UNIT, width * lanes), bf16),
                in_specs=[smem, vmem] + [anywhere] * 5 + [vmem, vmem],
                out_specs=vmem,
                scratch_shapes=[
                    *(pltpu.VMEM((pair, count, UNIT, wide), bf16) for count in counts1),
                    *(pltpu.VMEM((half, pair, count, UNIT, wide), bf16) for count in (cap1, near1)),
                    *(pltpu.VMEM((count * BATCH, UNIT, wide), bf16) for count in batches),
                    *(pltpu.VMEM((sum(counts2), UNIT, cut), bf16) for cut in cuts),
                    *(pltpu.VMEM((sum(counts2), UNIT, cut), bf16) for cut in cuts),
                    *(pltpu.VMEM((pair, lanes, held * share, UNIT, cut), bf16) for cut in cuts),
                    pltpu.VMEM((slots, prefix, HEAD), bf16),
                    pltpu.VMEM((slots, prefix, HEAD), bf16),
                    dma((planes, pair)), dma((planes, pair)), dma((4,)), dma((len(base),)),
                    dma((PIECES, planes)), dma((PIECES, planes)),
                    dma((PIECES, pair, lanes)), dma((PIECES, pair, lanes)),
                ],
                compiler_params=pltpu.CompilerParams(
                    collective_id=2 + level, has_side_effects=True, vmem_limit_bytes=ROOM
                ),
                name=f"packed_prefix_attention_{level}",
            )(*values)

        return run

    out = lax.switch(
        chosen.reshape(()), [branch(level) for level in range(len(levels))], *operands
    )
    return out.reshape(held, share * UNIT, width * lanes)


def fits(groups, lanes, queries, prefix_keys):
    held, rows, width = queries.shape
    pair = prefix_keys.shape[2] // HEAD
    if pair != 2 or groups // pair not in (2, 4) or groups % (2 * pair):
        return False
    if rows % (UNIT * lanes) or rows >= LANES:
        return False
    slots = pair * prefix_keys.shape[0]
    spots = 2 * groups * prefix_keys.shape[0]
    full_plane = CAPC * pair * pair * rows // UNIT
    room = groups // pair // 2 * full_plane + slots * (BATCH - 1)
    return max(groups * held, spots, full_plane) <= LANES and room <= 2 * LANES


def local(groups, lanes, queries, prefix_keys, *rest):
    form = packed if fits(groups, lanes, queries, prefix_keys) else padded
    return form(groups, lanes, queries, prefix_keys, *rest)


def solution(mesh):
    placed = (
        P("group", None, "tensor"),
        P("group", None, "tensor"),
        P("group", None, "tensor"),
        P(),
        P("group"),
        P("group"),
    )
    return jax.shard_map(
        functools.partial(local, mesh.shape["group"], mesh.shape["tensor"]),
        mesh=mesh, in_specs=placed, out_specs=P("group", "tensor", None), check_vma=False,
    )
```
